128 devices in a mesh: lat: 8 (over y, core), lon: 16 (over x, z).
Axes of the slice: x: 4, y: 4, z: 4, core: 2. Of those that a mesh axis runs over, the one named last changes fastest.
Arguments:
- obs_pert: bfloat16 [4096, 512, 256], P(('lat', 'lon')), may hold values from -3 to 3
- obs_weight: bfloat16 [4096, 512], P(('lat', 'lon')), may hold values from 0.5 to 2
- innovation: bfloat16 [4096, 512], P(('lat', 'lon')), may hold values from -6 to 6
- batch_len: int32 [128, 32], P(('lat', 'lon')), may hold values from 1 to 512, 10240 in all within a row
- batch_owner: int32 [4096, 1], P(('lat', 'lon')), may hold values from 0 to 15; in each aligned block of 32 rows (0 to 31, 32 to 63, ...) at most 4 rows name the same one
- batch_points: int32 [4096, 3], P(('lat', 'lon')), may hold values from 0 to 7, all different within a row
- batch_count: int32 [4096], P(('lat', 'lon')), may hold values from 1 to 3
- batch_taper: bfloat16 [4096, 3], P(('lat', 'lon')), may hold values from 0.25 to 1
- background: bfloat16 [64, 2048, 256], P('lat', 'lon'), may hold values from -6 to 6
- stencil: int32 [2, 64, 2048], P(None, 'lat', 'lon'), may hold values from 0 to 63, as said below
- frac: float32 [2, 64, 2048], P(None, 'lat', 'lon'), may hold values from 0 to 1
Outputs:
- analysis: bfloat16 [64, 2048, 256], P('lat', 'lon')
The draws below stay inside these ranges and needn't reach their ends.
Inputs may be any that keep to these rules, and one draw needn't show every extreme that they name: `batch_owner`: among the 32 batches held by one device, at most 4 share an owner, and in every draw some owner has exactly 4 of them. `batch_points`: the entries of a row are distinct; local point p of an owner is its point p // 4 along latitude and p % 4 along longitude. Only the first batch_count entries of a batch's row of batch_points and batch_taper count. `batch_len`: each row sums to 10240 and its largest entry is 512. For a cell in the block of cells a * 8 .. (a + 1) * 8 - 1 along latitude and c * 128 .. (c + 1) * 128 - 1 along longitude, stencil[0] lies in a * 2 - 1 .. (a + 1) * 2 - 1 and in 0 .. 14, and stencil[1] is (c * 4 - 1 + t) mod 64 for some t in 0 .. 4.
All inputs are finite; a program needn't handle non-finite values.
Results may differ from the reference program's by a relative error of at most 0.0059.
Values may be sent and summed in bfloat16 or wider, within the bound.
A program may use at most 128 MiB of HBM per device.

```python
import math
import jax
import jax.numpy as jnp
import numpy as np
from jax import lax

MEMBERS = 256
NOBS = 512
BAT_DEV = 32
CAP = 4
TOP = 3
PLAT = 2
PLON = 4
PTS_DEV = 8
CLAT = 8
CLON = 128
ITERS = 6
BATCHES = 4096
NPLAT = 16
NPLON = 64
NCLAT = 64
NCLON = 2048
N_LAT = 8
N_LON = 16


def draw_stencil(key, part):
    lat_key = jax.random.fold_in(key, 11)
    lon_key = jax.random.fold_in(key, 23)
    lat_block = jnp.arange(NCLAT, dtype=jnp.int32) // CLAT
    lon_block = jnp.arange(NCLON, dtype=jnp.int32) // CLON
    lat_step = jax.random.randint(lat_key, (NCLAT, NCLON), 0, PLAT + 1, dtype=jnp.int32)
    lon_step = jax.random.randint(lon_key, (NCLAT, NCLON), 0, PLON + 1, dtype=jnp.int32)
    lat_index = jnp.clip(lat_block[:, None] * PLAT - 1 + lat_step, 0, NPLAT - 2)
    lon_index = (lon_block[None, :] * PLON - 1 + lon_step) % NPLON
    return jnp.stack([lat_index, lon_index]).astype(jnp.int32)


def plant(drawn, rng, least, high):
    place = [jax.random.randint(jax.random.fold_in(rng, axis), (), 0, length) for axis, length in enumerate(drawn.shape)]
    widest = drawn.shape.index(max(drawn.shape))
    beside = place[:widest] + [(place[widest] + 1) % drawn.shape[widest]] + place[widest + 1:]
    return drawn.at[tuple(place)].set(least).at[tuple(beside)].set(high)


def shard_levels(rng, extent, cuts, least, top_value):
    def one(dim, shards_of):
        steps = jax.random.uniform(jax.random.fold_in(jax.random.fold_in(rng, 6), dim), (shards_of,), jnp.float32, least / len(cuts), top_value / len(cuts))
        return jnp.repeat(jnp.exp(steps), extent[dim] // shards_of).reshape((-1,) + (1,) * (len(extent) - dim - 1))

    loudness = one(*cuts[0])
    for cut in cuts[1:]:
        loudness = loudness * one(*cut)
    return loudness


def choose_distinct(stream_key, rows, count, top, lift):
    sequence = jax.random.permutation(jax.random.fold_in(stream_key, 1), count)
    pull = sequence
    for power in range(3):
        pull = pull * pull // count
    pull = pull * lift // count
    tickets = jax.random.randint(jax.random.fold_in(stream_key, 2), (rows, count), 0, 4096) + pull
    holders = jax.random.permutation(jax.random.fold_in(stream_key, 3), rows)[jnp.arange(count) % rows]
    tickets = jnp.where(jnp.arange(rows)[:, None] == holders[None, :], 1 << 14, tickets)
    priority = tickets * count + jnp.arange(count)
    return lax.top_k(priority.astype(jnp.int32), top)[1].astype(jnp.int32)


def split_up(number_of, total, bound, slope):
    portions = [(1 << 20) // math.isqrt(grade ** slope) + 1 for grade in range(2, number_of + 1)]
    surplus, holding = total - bound - (number_of - 1), [1] * (number_of - 1)
    while surplus > 0:
        candidates = [i for i in range(number_of - 1) if holding[i] < bound]
        mass, left = sum([portions[i] for i in candidates]), surplus
        for i in candidates:
            more = min(bound - holding[i], max(1, left * portions[i] // mass), surplus)
            holding[i] = holding[i] + more
            surplus = surplus - more
    return np.array([bound] + holding)


def ragged(stream_key, number_of, total, limit, skew):
    if number_of == 2:
        one = jax.random.randint(stream_key, (), max(1, total - limit), min(limit, total - 1) + 1)
        return jnp.stack([one, total - one])
    sizes = jnp.asarray(split_up(number_of, total, limit, skew), jnp.int32)
    couples = (number_of - 1) // 2
    giver, receiver = sizes[1:1 + 2 * couples:2], sizes[2:2 + 2 * couples:2]
    room = jnp.minimum(giver - 1, limit - receiver)
    moved = jax.random.randint(jax.random.fold_in(stream_key, 1), (couples,), 0, 1 << 20) % (room + 1)
    sizes = sizes.at[1:1 + 2 * couples:2].set(giver - moved).at[2:2 + 2 * couples:2].set(receiver + moved)
    return sizes[jax.random.permutation(jax.random.fold_in(stream_key, 2), number_of)]


def assign_block(own_key, own, number, rows, number_of, top, bound, lean):
    order = jax.random.permutation(own_key, number_of)
    crowded, ordinary = load_shares(number_of, rows * top, bound, lean, True), load_shares(number_of, rows * top, bound, lean, False)
    places = jnp.arange(number_of)

    def named(sizes, offset_by):
        used = int((sizes > 0).sum())
        fixed = max(1, used // 4)
        shifted = fixed + (places - fixed + offset_by * (used - fixed)) % max(1, number_of - fixed)
        return jnp.zeros((number_of,), jnp.int32).at[order[jnp.where(places < fixed, places, shifted)]].set(jnp.asarray(sizes, jnp.int32))

    sizes = jnp.where(number % 4 == 0, named(crowded, number // 4), named(ordinary, number - number // 4 - 1))
    mixed = jax.random.permutation(jax.random.fold_in(own, 3), number_of)
    giver, receiver = mixed[0:number_of // 2 * 2:2], mixed[1:number_of // 2 * 2:2]
    room = jnp.minimum(sizes[giver] - 1, bound - sizes[receiver]) // 2
    room = jnp.where((giver == order[0]) | (receiver == order[0]) | (sizes[receiver] == 0), 0, jnp.maximum(room, 0))
    shifted = jax.random.randint(jax.random.fold_in(own, 4), (number_of // 2,), 0, 1 << 20) % (room + 1)
    sizes = sizes.at[giver].add(-shifted).at[receiver].add(shifted)
    items = jnp.searchsorted(jnp.cumsum(sizes), jnp.arange(rows * top), side="right").astype(jnp.int32)
    table = items.reshape(top, rows).T
    table = table[jax.random.permutation(jax.random.fold_in(own, 1), rows)]
    offset_by = jax.random.randint(jax.random.fold_in(own, 2), (rows, 1), 0, top)
    return jnp.take_along_axis(table, (jnp.arange(top)[None, :] + offset_by) % top, axis=1)


def load_shares(count, total, reach, slope, full):
    portions = [(1 << 20) // math.isqrt(grade ** slope) + 1 for grade in range(1, count + 1)]
    largest = reach if full else min(reach, max(-(-total // count), total * portions[0] // sum(portions)))
    least = 1 if total - largest >= count - 1 else 0
    given, rest = [largest] + [least] * (count - 1), total - largest - least * (count - 1)
    while rest > 0:
        free = [i for i in range(1, count) if given[i] < largest] or [i for i in range(1, count) if given[i] < reach]
        pool, remaining = sum([portions[i] for i in free]), rest
        for i in free:
            addition = min(reach - given[i], max(1, remaining * portions[i] // pool), rest)
            given[i] = given[i] + addition
            rest = rest - addition
    return np.array(given)


def bell_draw(own_key, shape, scale, bound, cuts=(), kind=jnp.bfloat16):
    values = scale * jax.random.normal(own_key, shape, jnp.float32)
    if cuts:
        values = values * shard_levels(own_key, shape, cuts, -0.22, 0.18)
    return jnp.clip(values, -bound, bound).astype(kind)


def setup_inputs(seed: int = 0) -> dict:
    key_list = jax.random.split(jax.random.key(seed), 12)
    obs_pert = bell_draw(key_list[0], (BATCHES, NOBS, MEMBERS), 0.5, 3.0, ((0, 128),))
    obs_weight = jnp.clip(jnp.exp(math.log(2.0) - 1.3862944 * jax.random.uniform(key_list[1], (BATCHES, NOBS), jnp.float32) ** shard_levels(key_list[1], (BATCHES, NOBS), ((0, 128),), -0.2, 0.2)), 0.5, 2.0).astype(jnp.bfloat16)
    innovation = bell_draw(key_list[2], (BATCHES, NOBS), 1.0, 6.0, ((0, 128),))
    batch_len = jax.vmap(lambda own: ragged(own, BAT_DEV, BAT_DEV * NOBS * 5 // 8, NOBS, 2))(jax.random.split(key_list[3], (N_LAT * N_LON))).reshape((N_LAT * N_LON, BAT_DEV)).astype(jnp.int32)
    batch_owner_keys = jax.random.split(jax.random.fold_in(key_list[4], 1), BATCHES // BAT_DEV)
    batch_owner_turns = jax.random.permutation(jax.random.fold_in(key_list[4], 3), BATCHES // BAT_DEV)
    batch_owner = jax.vmap(lambda own, number: assign_block(jax.random.fold_in(key_list[4], 2), own, number, BAT_DEV, N_LON, 1, CAP, 2))(batch_owner_keys, batch_owner_turns).reshape((BATCHES, 1))
    batch_points = choose_distinct(key_list[5], BATCHES, PTS_DEV, TOP, 0)
    batch_count = plant(jax.random.randint(key_list[6], (BATCHES,), 1, TOP + 1), jax.random.fold_in(key_list[6], 1), 1, TOP).astype(jnp.int32)
    batch_taper = jnp.clip(jnp.exp(math.log(1.0) - 1.3862944 * jax.random.uniform(key_list[7], (BATCHES, TOP), jnp.float32) ** shard_levels(key_list[7], (BATCHES, TOP), ((0, 128),), -0.2, 0.2)), 0.25, 1.0).astype(jnp.bfloat16)
    background = bell_draw(key_list[8], (NCLAT, NCLON, MEMBERS), 1.0, 6.0, ((0, 8), (1, 16)))
    stencil = draw_stencil(jax.random.fold_in(key_list[11], 71), 0)
    frac = jnp.clip(1.0 * jax.random.uniform(key_list[10], (2, NCLAT, NCLON), jnp.float32) ** shard_levels(key_list[10], (2, NCLAT, NCLON), ((1, 8), (2, 16)), -0.2, 0.2), 0.0, 1.0)
    return dict(obs_pert=obs_pert, obs_weight=obs_weight, innovation=innovation, batch_len=batch_len, batch_owner=batch_owner, batch_points=batch_points, batch_count=batch_count, batch_taper=batch_taper, background=background, stencil=stencil, frac=frac)


def one_batch(item):
    pert_rows, weight_rows, innov_rows, length = item
    live_rows = (jnp.arange(NOBS) < length).astype(jnp.float32)
    kept = weight_rows.astype(jnp.float32) * live_rows
    scaled = (kept[:, None] * pert_rows.astype(jnp.float32)).astype(jnp.bfloat16)
    batch_gram = jnp.dot(scaled.T, pert_rows, preferred_element_type=jnp.float32).astype(jnp.bfloat16)
    batch_proj = jnp.dot(innov_rows, scaled, preferred_element_type=jnp.float32).astype(jnp.bfloat16)
    return (batch_gram, batch_proj)

def point_weights(batch_points, batch_count, batch_taper):
    listed = jnp.arange(TOP, dtype=jnp.int32)
    valid = listed[None, :] < batch_count[:, None]
    onehot = batch_points[:, :, None] == jnp.arange(PTS_DEV, dtype=jnp.int32)[None, None, :]
    picked = jnp.where(valid[:, :, None] & onehot, batch_taper.astype(jnp.float32)[:, :, None], jnp.float32(0.0))
    return lax.optimization_barrier(jnp.sum(picked, axis=1)).astype(jnp.bfloat16)

def analysis_transform(item):
    total, shift = item
    identity = jnp.eye(MEMBERS, dtype=jnp.float32)
    system = total + (MEMBERS - 1) * identity
    scale = jnp.sqrt(jnp.sum(system * system))
    iterate = system / scale
    inverse_root = identity
    for sweep in range(ITERS):
        factor = 1.5 * identity - 0.5 * jnp.dot(inverse_root, iterate, precision=lax.Precision.HIGHEST)
        iterate = jnp.dot(iterate, factor, precision=lax.Precision.HIGHEST)
        inverse_root = jnp.dot(factor, inverse_root, precision=lax.Precision.HIGHEST)
    inner = jnp.dot(inverse_root, shift, precision=lax.Precision.HIGHEST)
    mean_weight = jnp.dot(inverse_root, inner, precision=lax.Precision.HIGHEST) / scale
    result = jnp.sqrt((MEMBERS - 1) / scale) * inverse_root + mean_weight[:, None]
    return result.astype(jnp.bfloat16)

def interp_weights(stencil, frac, lat_pos, lon_pos, point_cols):
    row_off = stencil[0] - (lat_pos * PLAT - 1)
    col_off = (stencil[1] - lon_pos * PLON + 1) % point_cols
    lat_frac = frac[0].reshape(-1)[:, None]
    lon_frac = frac[1].reshape(-1)[:, None]
    corner_id = (row_off * (PLON + 2) + col_off).reshape(-1)[:, None]
    all_ids = jnp.arange((PLAT + 2) * (PLON + 2), dtype=jnp.int32)[None, :]
    zero_val = jnp.float32(0.0)
    weights = jnp.where(corner_id == all_ids, (1.0 - lat_frac) * (1.0 - lon_frac), zero_val)
    weights = weights + jnp.where(corner_id + (PLON + 2) == all_ids, lat_frac * (1.0 - lon_frac), zero_val)
    weights = weights + jnp.where(corner_id + 1 == all_ids, (1.0 - lat_frac) * lon_frac, zero_val)
    weights = weights + jnp.where(corner_id + (PLON + 3) == all_ids, lat_frac * lon_frac, zero_val)
    return weights

def reference(obs_pert, obs_weight, innovation, batch_len, batch_owner, batch_points, batch_count, batch_taper, background, stencil, frac):
    lengths = batch_len.reshape(-1)
    grams, projs = lax.map(one_batch, (obs_pert, obs_weight, innovation, lengths))
    coef = point_weights(batch_points, batch_count, batch_taper)
    band_size = N_LON * BAT_DEV
    owners = batch_owner[:, 0].reshape(N_LAT, band_size)
    coef_rows = coef.reshape(N_LAT, band_size, PTS_DEV)
    gram_rows = grams.reshape(N_LAT, band_size, MEMBERS * MEMBERS)
    proj_rows = projs.reshape(N_LAT, band_size, MEMBERS)

    def one_band(item):
        band_owner, band_coef, band_gram, band_proj = item
        local = jnp.arange(PTS_DEV, dtype=jnp.int32)
        target = (local // PLON)[None, :] * NPLON + band_owner[:, None] * PLON + (local % PLON)[None, :]
        hit_table = target[None, :, :] == jnp.arange(PLAT * NPLON, dtype=jnp.int32)[:, None, None]
        mixing = lax.optimization_barrier(jnp.sum(jnp.where(hit_table, band_coef.astype(jnp.float32)[None], jnp.float32(0.0)), axis=2))
        totals = jnp.dot(mixing, band_gram.astype(jnp.float32), precision=lax.Precision.HIGHEST)
        shifts = jnp.dot(mixing, band_proj.astype(jnp.float32), precision=lax.Precision.HIGHEST)
        return (totals, shifts)
    totals, shifts = lax.map(one_band, (owners, coef_rows, gram_rows, proj_rows))
    transforms = lax.map(analysis_transform, (totals.reshape(-1, MEMBERS, MEMBERS), shifts.reshape(-1, MEMBERS)))
    transforms = transforms.reshape(NPLAT, NPLON, MEMBERS, MEMBERS)
    mean_field = lax.optimization_barrier(jnp.mean(background.astype(jnp.float32), axis=-1))
    deviation = (background.astype(jnp.float32) - mean_field[..., None]).astype(jnp.bfloat16)
    zero_idx = jnp.zeros((), jnp.int32)

    def one_tile(tile):
        lat_pos = (tile // N_LON).astype(jnp.int32)
        lon_pos = (tile % N_LON).astype(jnp.int32)
        rows = (lat_pos * PLAT - 1 + jnp.arange(PLAT + 2, dtype=jnp.int32)) % NPLAT
        cols = (lon_pos * PLON - 1 + jnp.arange(PLON + 2, dtype=jnp.int32)) % NPLON
        window = transforms[rows][:, cols].reshape(-1, MEMBERS, MEMBERS)
        cells = lax.dynamic_slice(deviation, (lat_pos * CLAT, lon_pos * CLON, zero_idx), (CLAT, CLON, MEMBERS))
        tile_mean = lax.dynamic_slice(mean_field, (lat_pos * CLAT, lon_pos * CLON), (CLAT, CLON))
        tile_sten = lax.dynamic_slice(stencil, (zero_idx, lat_pos * CLAT, lon_pos * CLON), (2, CLAT, CLON))
        tile_frac = lax.dynamic_slice(frac, (zero_idx, lat_pos * CLAT, lon_pos * CLON), (2, CLAT, CLON))
        weights = interp_weights(tile_sten, tile_frac, lat_pos, lon_pos, NPLON)
        products = jnp.einsum('ck,jkl->cjl', cells.reshape(-1, MEMBERS).astype(jnp.float32), window.astype(jnp.float32), precision=lax.Precision.HIGHEST)
        mixed = jnp.einsum('cj,cjl->cl', weights, products, precision=lax.Precision.HIGHEST)
        return (tile_mean.reshape(-1)[:, None] + mixed).astype(jnp.bfloat16)
    tiles = lax.map(one_tile, jnp.arange(N_LAT * N_LON, dtype=jnp.int32))
    tiles = tiles.reshape(N_LAT, N_LON, CLAT, CLON, MEMBERS)
    return jnp.transpose(tiles, (0, 2, 1, 3, 4)).reshape(NCLAT, NCLON, MEMBERS)
```

```python
import jax
import jax.numpy as jnp
from jax import lax
from jax.experimental import pallas as pl
from jax.experimental.pallas import tpu as pltpu
from jax.sharding import PartitionSpec as P

MEMBERS = 256
NOBS = 512
BAT = 32
TOP = 3
PTS = 8
ITERS = 6
HALF = 128
MESH = pl.DeviceIdType.MESH
F32 = jnp.float32
BF16 = jnp.bfloat16
COPIES = 64


def iota(shape, dim):
    return lax.broadcasted_iota(jnp.int32, shape, dim)


def dot(a, b):
    return jnp.dot(a, b, preferred_element_type=F32)


def dot_first(a, b):
    return lax.dot_general(a, b, (((0,), (0,)), ((), ())), preferred_element_type=F32)


def relative_bits(owner, me):
    ox, oz, mx, mz = owner // 4, owner % 4, me // 4, me % 4
    gx = (ox ^ (ox >> 1)) ^ (mx ^ (mx >> 1))
    gz = (oz ^ (oz >> 1)) ^ (mz ^ (mz >> 1))
    return (gx & 1, gx >> 1, gz & 1, gz >> 1)


def moments_kernel(
    owner_s,
    points_s,
    count_s,
    len_s,
    weight_ref,
    innov_ref,
    taper_ref,
    pert_hbm,
    packed_ref,
    extra_ref,
    coef_ref,
    pert,
    wide_w,
    wide_i,
    acc,
    extra_f,
    rows_i,
    used_s,
    pos_s,
    sems,
):
    me = lax.axis_index("lon")

    def fetch(b, part):
        rows = pl.ds(part * 256, 256)
        return pltpu.make_async_copy(pert_hbm.at[b, rows], pert.at[b, rows], sems.at[part, b])

    def start(b, carry):
        fetch(b, 0).start()

        @pl.when(len_s[0, b] > 256)
        def _():
            fetch(b, 1).start()

        return carry

    lax.fori_loop(0, BAT, start, 0)

    packed_ref[...] = jnp.zeros(packed_ref.shape, BF16)
    extra_f[...] = jnp.zeros(extra_f.shape, F32)
    wide_w[...] = weight_ref[...].astype(F32)
    wide_i[...] = innov_ref[...].astype(F32)
    for o in range(16):
        used_s[o] = 0

    def place(b, carry):
        owner = owner_s[b, 0]
        rank = used_s[owner]
        used_s[owner] = rank + 1
        bits = relative_bits(owner, me)
        for k in range(4):
            d = [bits[(k + i) % 4] for i in range(4)]
            pos_s[k, b] = d[0] * 8 + d[1] * 4 + d[2] * 2 + d[3]
        pos_s[4, b] = rank
        full = lambda v: jnp.full((1, HALF), v, jnp.int32)
        rows_i[0, pl.ds(b, 1), :] = full(owner * 4 + rank)
        rows_i[1, pl.ds(b, 1), :] = full(count_s[b])
        for j in range(TOP):
            rows_i[2 + j, pl.ds(b, 1), :] = full(points_s[b, j])
        return carry

    lax.fori_loop(0, BAT, place, 0)

    lane = iota((BAT, HALF), 1)
    taper = taper_ref[...].astype(F32)
    coef = jnp.zeros((BAT, HALF), F32)
    for j in range(TOP):
        hit = (rows_i[2 + j] == lane) & (rows_i[1] > j)
        coef = coef + jnp.where(hit, taper[:, j : j + 1], 0.0)
    spot = jnp.where(rows_i[0] == lane, 1.0, 0.0)
    coef_ref[...] = dot_first(coef.astype(BF16), spot.astype(BF16))[0:PTS, :]

    row, col = iota((HALF, HALF), 0), iota((HALF, HALF), 1)
    first = iota((16, 256), 0)

    def product(b, part, length):
        p = pert[b, part * 256 : part * 256 + 256, :]
        cols = slice(part * 256, part * 256 + 256)
        live = (iota((1, 256), 1) + part * 256) < length
        w = jnp.where(live, wide_w[pl.ds(b, 1), cols], 0.0)
        wi = w * wide_i[pl.ds(b, 1), cols]
        high = wi.astype(BF16).astype(F32)
        low = wi - high
        tail = jnp.where(first == 0, high, jnp.where(first == 1, low, 0.0)).astype(BF16)
        scaled = (p.T.astype(F32) * w).astype(BF16)
        return dot(jnp.concatenate([scaled, tail], axis=0), p)

    def one(b, carry):
        length = len_s[0, b]
        fetch(b, 0).wait()
        acc[...] = product(b, 0, length)

        @pl.when(length > 256)
        def _():
            fetch(b, 1).wait()
            acc[...] += product(b, 1, length)

        corner = acc[HALF:256, HALF:256]
        left = jnp.where(col >= row, acc[0:HALF, 0:HALF], corner)
        top = jnp.concatenate([left, acc[0:HALF, HALF:256]], axis=1).astype(BF16)
        rank = pos_s[4, b]
        for k in range(4):
            for rc in range(2):
                at = 32 * k + 16 * rc
                packed_ref[k, pos_s[k, b], rc, rank] = top[at : at + 16, :]
        proj = acc[256:257, :] + acc[257:258, :]
        base = pos_s[0, b] * 16 + rank * 4
        extra_f[pl.ds(base, 1), :] = jnp.sum(
            jnp.where(col == row, corner, 0.0), axis=0, keepdims=True
        )
        extra_f[pl.ds(base + 1, 1), :] = proj[:, 0:HALF]
        extra_f[pl.ds(base + 2, 1), :] = proj[:, HALF:256]
        return carry

    lax.fori_loop(0, BAT, one, 0)
    extra_ref[...] = extra_f[...].astype(BF16).reshape(extra_ref.shape)


def moments(obs_pert, obs_weight, innovation, batch_len, owner, points, count, taper):
    smem = pl.BlockSpec(memory_space=pltpu.SMEM)
    vmem = pl.BlockSpec(memory_space=pltpu.VMEM)
    return pl.pallas_call(
        moments_kernel,
        out_shape=(
            jax.ShapeDtypeStruct((4, 16, 2, 4, 16, 256), BF16),
            jax.ShapeDtypeStruct((16, 16, HALF), BF16),
            jax.ShapeDtypeStruct((PTS, HALF), F32),
        ),
        in_specs=[smem, smem, smem, smem, vmem, vmem, vmem, pl.BlockSpec(memory_space=pl.ANY)],
        out_specs=(vmem, vmem, vmem),
        scratch_shapes=[
            pltpu.VMEM((BAT, NOBS, MEMBERS), BF16),
            pltpu.VMEM((BAT, NOBS), F32),
            pltpu.VMEM((BAT, NOBS), F32),
            pltpu.VMEM((272, 256), F32),
            pltpu.VMEM((256, HALF), F32),
            pltpu.VMEM((5, BAT, HALF), jnp.int32),
            pltpu.SMEM((16,), jnp.int32),
            pltpu.SMEM((5, BAT), jnp.int32),
            pltpu.SemaphoreType.DMA((2, BAT)),
        ],
        compiler_params=pltpu.CompilerParams(vmem_limit_bytes=40 << 20),
        name="moments",
    )(owner, points, count, batch_len, obs_weight, innovation, taper, obs_pert)


def flip(x, z, dim):
    if dim == 0:
        return x + 1 - 2 * (x % 2), z
    if dim == 1:
        return 3 - x, z
    if dim == 2:
        return x, z + 1 - 2 * (z % 2)
    return x, 3 - z


def root_iteration(e_s, eb_s, z_s, scal, k):
    new = []
    for p in range(4):
        m, z = scal[p]
        f = 1.5 - 0.5 * m
        e = e_s[p]
        eb = eb_s[p]
        if k == 0:
            z_s[p] = -0.5 * e
        else:
            r = z_s[p]
            z_s[p] = f * r - 0.5 * (dot(r.astype(BF16), eb) + z * e)
        if k < ITERS - 1:
            g = m * f
            h = (f - 0.5 * m) * e - 0.5 * dot(eb, eb)
            e_new = f * h - 0.5 * (g * e + dot(h.astype(BF16), eb))
            e_s[p] = e_new
            eb_s[p] = e_new.astype(BF16)
        new.append((m * f * f, z * f))
    return new


def exchange_kernel(
    packed,
    extra,
    coef,
    window_out,
    held,
    coef_n,
    coef_d,
    send3,
    recv3,
    send4,
    recv4,
    mine1,
    total,
    xheld,
    xsend3,
    xrecv3,
    xsend4,
    xrecv4,
    xmine1,
    xtotal,
    e_s,
    eb_s,
    z_s,
    window,
    local_sems,
    out_sems,
    send_sems,
    recv_sems,
):
    lat, lon = lax.axis_index("lat"), lax.axis_index("lon")
    x, z = lon // 4, lon % 4

    def to(dim):
        hx, hz = flip(x, z, dim % 4)
        return (lat, hx * 4 + hz)

    east, west = (lat, (lon + 1) % 16), (lat, (lon + 15) % 16)
    south, north = ((lat + 1) % 8, lon), ((lat + 7) % 8, lon)

    barrier = pltpu.get_barrier_semaphore()
    peers = [to(d) for d in range(4)] + [east, west, south, north]
    for peer in peers:
        pl.semaphore_signal(barrier, inc=1, device_id=peer, device_id_type=MESH)
    own = [
        pltpu.make_async_copy(packed.at[k, 0:8], held.at[k, :, :, 0], local_sems.at[k])
        for k in range(4)
    ]
    own.append(pltpu.make_async_copy(extra.at[0:8], xheld.at[:, 0], local_sems.at[4]))
    for c in own:
        c.start()
    pl.semaphore_wait(barrier, len(peers))

    used = []

    def push(src, dst, peer):
        n = len(used)
        c = pltpu.make_async_remote_copy(
            src_ref=src,
            dst_ref=dst,
            send_sem=send_sems.at[n],
            recv_sem=recv_sems.at[n],
            device_id=peer,
            device_id_type=MESH,
        )
        c.start()
        used.append(c)
        return c

    cn = [push(coef, coef_n.at[k], to(k)) for k in range(4)]
    s1a = [push(packed.at[k, 12:16], held.at[k, 4:8, :, 1], to(k)) for k in range(4)]
    x1 = push(extra.at[8:16], xheld.at[:, 1], to(0))
    s1b = [push(packed.at[k, 8:12], held.at[k, 0:4, :, 1], to(k)) for k in range(4)]

    for c in own:
        c.wait()
    for k in range(4):
        cn[k].wait_recv()
    cd = [push(coef_n.at[k], coef_d.at[k], to(k + 1)) for k in range(4)]
    s2a, s2b = [], []
    for k in range(4):
        s1a[k].wait_recv()
        s2a.append(push(held.at[k, 6:8, :, 0:2], held.at[k, 2:4, :, 2:4], to(k + 1)))
    for k in range(4):
        s2b.append(push(held.at[k, 4:6, :, 0:2], held.at[k, 0:2, :, 2:4], to(k + 1)))
    x1.wait_recv()
    x2 = push(xheld.at[4:8, 0:2], xheld.at[0:4, 2:4], to(1))

    def sources(k):
        rows = [coef[...], coef_n[k], coef_n[(k + 1) % 4], coef_d[k]]
        return jnp.concatenate(rows, axis=0).astype(BF16)

    def served(k, pos):
        sx, sz = x, z
        if pos & 2:
            sx, sz = flip(sx, sz, (k + 2) % 4)
        if pos & 1:
            sx, sz = flip(sx, sz, (k + 3) % 4)
        return sx * 4 + sz

    def spread(k, pos, width, each):
        lane = iota((HALF, width), 1)
        pick = jnp.where(
            iota((HALF, width), 0) == served(k, pos) * 4 + (lane // each) % 4, 1.0, 0.0
        ).astype(BF16)
        every = dot(sources(k), pick)
        lane8 = iota((8, width), 1) // (4 * each)
        out = jnp.zeros((8, width), F32)
        for j in range(4):
            out = out + jnp.where(lane8 == j, every[8 * j : 8 * j + 8, :], 0.0)
        return out

    def expand(weights, rows, each):
        width = weights.shape[1]
        keep = iota((rows, width), 1) % each == iota((rows, width), 0)
        blocks = [
            jnp.where(keep, jnp.broadcast_to(weights[p : p + 1, :], (rows, width)), 0.0)
            for p in range(PTS)
        ]
        return jnp.concatenate(blocks, axis=0).astype(BF16)

    def merged(k, pos):
        lhs = expand(spread(k, pos, 256, 16), 16, 16)
        return [
            dot(lhs, held[k, pos, rc].reshape(256, 256)).reshape(PTS, 16, 256) for rc in range(2)
        ]

    def xmerged(pos):
        lhs = expand(spread(0, pos, HALF, 4), 8, 4)
        return dot(lhs[:, 0:64], xheld[pos].reshape(64, HALF))

    s3a, s3b = [], []
    for k in range(4):
        cd[k].wait_recv()
        s1b[k].wait_recv()
    for pos in (3, 2):
        for k in range(4):
            if pos == 3:
                s2a[k].wait_recv()
            for rc, value in enumerate(merged(k, pos)):
                send3[k, pos - 2, :, 16 * rc : 16 * rc + 16, :] = value.astype(BF16)
            if pos == 3:
                s3a.append(push(send3.at[k, 1], recv3.at[k, 1], to(k + 2)))
            else:
                for h in range(2):
                    span = pl.ds(4 * h, 4)
                    s3b.append(push(send3.at[k, 0, span], recv3.at[k, 0, span], to(k + 2)))
    x2.wait_recv()
    for pos in (3, 2):
        xsend3[pos - 2] = xmerged(pos).astype(BF16)
    x3 = push(xsend3, xrecv3, to(2))

    for pos in (1, 0):
        for k in range(4):
            if pos == 1:
                s2b[k].wait_recv()
            for rc, value in enumerate(merged(k, pos)):
                if pos == 1:
                    mine1[k, :, 16 * rc : 16 * rc + 16, :] = value
                else:
                    at = 32 * k + 16 * rc
                    total[:, at : at + 16, :] = value
    xmine1[...] = xmerged(1)
    xtotal[...] = xmerged(0)

    s4 = []
    for k in range(4):
        s3a[k].wait_recv()
        send4[k] = (mine1[k] + recv3[k, 1].astype(F32)).astype(BF16)
        s4.append(push(send4.at[k, 0:4], recv4.at[k, 0:4], to(k + 3)))
    x3.wait_recv()
    xsend4[...] = (xmine1[...] + xrecv3[1].astype(F32)).astype(BF16)
    x4 = push(xsend4, xrecv4, to(3))
    for k in range(4):
        s4.append(push(send4.at[k, 4:8], recv4.at[k, 4:8], to(k + 3)))
    x4.wait_recv()
    xtotal[...] += xrecv3[0].astype(F32) + xrecv4[...].astype(F32)

    row, col = iota((HALF, HALF), 0), iota((HALF, HALF), 1)
    outs = []

    def keep(n):
        c = pltpu.make_async_copy(window.at[n], window_out.at[n], out_sems.at[n])
        c.start()
        outs.append(c)

    side = []
    for h in range(2):
        scal, scales = [], []
        for k in range(4):
            s3b[2 * k + h].wait_recv()
            s4[4 * h + k].wait_recv()
        for i in range(4):
            p = 4 * h + i
            for k in range(4):
                total[p, 32 * k : 32 * k + 32, :] += recv3[k, 0, p].astype(F32) + recv4[
                    k, p
                ].astype(F32)
            left, right = total[p, :, 0:HALF], total[p, :, HALF:256]
            turned = left.T
            eye = jnp.where(row == col, float(MEMBERS - 1), 0.0)
            a = jnp.where(col >= row, left, turned) + eye
            c = jnp.where(col < row, left, turned)
            c = jnp.where(col == row, xtotal[8 * p : 8 * p + 1, :], c) + eye
            square = jnp.sum(a * a + c * c + 2.0 * (right * right), keepdims=True)
            trace = jnp.sum(jnp.where(row == col, a + c, 0.0), keepdims=True)
            scale = jnp.sqrt(square)
            inverse = 1.0 / scale
            mean = trace * (1.0 / MEMBERS)
            off = jnp.where(row == col, mean, 0.0)
            a, c, b = (a - off) * inverse, (c - off) * inverse, right * inverse
            e_s[i] = jnp.concatenate(
                [jnp.concatenate([a, b], axis=1), jnp.concatenate([b.T, c], axis=1)], axis=0
            )
            eb_s[i] = e_s[i].astype(BF16)
            scal.append((mean * inverse, jnp.ones((1, 1), F32)))
            scales.append(scale)
        for k in range(ITERS):
            scal = root_iteration(e_s, eb_s, z_s, scal, k)
        for i in range(4):
            p = 4 * h + i
            zd = scal[i][1]
            r = z_s[i]
            high = r.astype(BF16)
            low = (r - high.astype(F32)).astype(BF16)

            def apply(v):
                vh = v.astype(BF16).astype(F32)
                first = iota((16, 256), 0)
                both = jnp.where(first == 0, vh, jnp.where(first == 1, v - vh, 0.0)).astype(BF16)
                w = dot(both, high) + dot(both, low)
                return zd * v + w[0:1, :] + w[1:2, :]

            shift = jnp.concatenate(
                [xtotal[8 * p + 1 : 8 * p + 2, :], xtotal[8 * p + 2 : 8 * p + 3, :]], axis=1
            )
            mw = apply(apply(shift)) / scales[i]
            amp = jnp.sqrt(float(MEMBERS - 1) / scales[i])
            big = iota((256, 256), 0) == iota((256, 256), 1)
            full = amp * (r + jnp.where(big, zd, 0.0)) + mw
            slot = (h + 1) * 6 + i + 1
            window[slot] = full.astype(BF16)
            if i == 0:
                side.append(push(window.at[slot], window.at[(h + 1) * 6 + 5], west))
            if i == 3:
                side.append(push(window.at[slot], window.at[(h + 1) * 6], east))
            if h == 0:
                push(window.at[slot], window.at[18 + i + 1], north)
            else:
                push(window.at[slot], window.at[i + 1], south)
            keep(slot)
    for h in range(2):
        for j in range(2):
            side[2 * h + j].wait_recv()
            at = (h + 1) * 6 + (5 if j == 0 else 0)
            column = 5 if j == 0 else 0
            if h == 0:
                push(window.at[at], window.at[18 + column], north)
            else:
                push(window.at[at], window.at[column], south)
            keep(at)
    done = set(id(c) for c in cn + cd + s1a + s1b + s2a + s2b + s3a + s3b + s4 + side)
    done |= set(id(c) for c in (x1, x2, x3, x4))
    for c in used:
        if id(c) not in done:
            c.wait_recv()
    for n in list(range(6)) + list(range(18, 24)):
        keep(n)
    for c in outs:
        c.wait()
    for c in used:
        c.wait_send()


def exchange(packed, extra, coef):
    vmem = pl.BlockSpec(memory_space=pltpu.VMEM)
    hbm = pl.BlockSpec(memory_space=pl.ANY)
    return pl.pallas_call(
        exchange_kernel,
        out_shape=jax.ShapeDtypeStruct((24, 256, 256), BF16),
        in_specs=[hbm, hbm, vmem],
        out_specs=hbm,
        scratch_shapes=[
            pltpu.VMEM((4, 8, 2, 4, 4, 16, 256), BF16),
            pltpu.VMEM((4, PTS, HALF), F32),
            pltpu.VMEM((4, PTS, HALF), F32),
            pltpu.VMEM((4, 2, PTS, 32, 256), BF16),
            pltpu.VMEM((4, 2, PTS, 32, 256), BF16),
            pltpu.VMEM((4, PTS, 32, 256), BF16),
            pltpu.VMEM((4, PTS, 32, 256), BF16),
            pltpu.VMEM((4, PTS, 32, 256), F32),
            pltpu.VMEM((PTS, HALF, 256), F32),
            pltpu.VMEM((8, 4, 16, HALF), BF16),
            pltpu.VMEM((2, 64, HALF), BF16),
            pltpu.VMEM((2, 64, HALF), BF16),
            pltpu.VMEM((64, HALF), BF16),
            pltpu.VMEM((64, HALF), BF16),
            pltpu.VMEM((64, HALF), F32),
            pltpu.VMEM((64, HALF), F32),
            pltpu.VMEM((4, 256, 256), F32),
            pltpu.VMEM((4, 256, 256), BF16),
            pltpu.VMEM((4, 256, 256), F32),
            pltpu.VMEM((24, 256, 256), BF16),
            pltpu.SemaphoreType.DMA((5,)),
            pltpu.SemaphoreType.DMA((24,)),
            pltpu.SemaphoreType.DMA((COPIES,)),
            pltpu.SemaphoreType.DMA((COPIES,)),
        ],
        compiler_params=pltpu.CompilerParams(
            collective_id=0, has_side_effects=True, vmem_limit_bytes=48 << 20
        ),
        name="exchange",
    )(packed, extra, coef)


def analysis_kernel(background, stencil, frac, window, out, weights, folded):
    lat, lon = lax.axis_index("lat"), lax.axis_index("lon")
    row_off = stencil[0] - (lat * 2 - 1)
    col_off = (stencil[1] - lon * 4 + 1) % 64
    corner = row_off * 6 + col_off
    fy, fx = frac[0], frac[1]
    kinds = (
        (0, (1.0 - fy) * (1.0 - fx)),
        (6, fy * (1.0 - fx)),
        (1, (1.0 - fy) * fx),
        (7, fy * fx),
    )
    for j in range(24):
        value = jnp.zeros((8, HALF), F32)
        for add, weight in kinds:
            value = value + jnp.where(corner + add == j, weight, 0.0)
        weights[j] = value
    for t in range(4):
        cells = background[2 * t : 2 * t + 2].reshape(256, 256)
        turned = cells.T.astype(F32)
        mean = jnp.sum(turned, axis=0, keepdims=True) * (1.0 / MEMBERS)
        deviation = (turned - mean).astype(BF16).astype(F32)
        mixed = jnp.zeros((256, 256), F32)
        for j in range(24):
            w = jnp.concatenate([weights[j, 2 * t : 2 * t + 1], weights[j, 2 * t + 1 : 2 * t + 2]], axis=1)
            mixed = mixed + dot(window[j], (deviation * w).astype(BF16))
        out[2 * t : 2 * t + 2] = (mixed + mean).T.astype(BF16).reshape(2, HALF, 256)


def analyse(background, stencil, frac, window):
    vmem = pl.BlockSpec(memory_space=pltpu.VMEM)
    return pl.pallas_call(
        analysis_kernel,
        out_shape=jax.ShapeDtypeStruct((8, HALF, 256), BF16),
        in_specs=[vmem] * 4,
        out_specs=vmem,
        scratch_shapes=[
            pltpu.VMEM((24, 8, HALF), F32),
            pltpu.VMEM((16, HALF), F32),
        ],
        compiler_params=pltpu.CompilerParams(vmem_limit_bytes=40 << 20),
        name="analysis",
    )(background, stencil, frac, window)


def on_device(
    obs_pert,
    obs_weight,
    innovation,
    batch_len,
    batch_owner,
    batch_points,
    batch_count,
    batch_taper,
    background,
    stencil,
    frac,
):
    packed, extra, coef = moments(
        obs_pert,
        obs_weight,
        innovation,
        batch_len,
        batch_owner,
        batch_points,
        batch_count,
        batch_taper,
    )
    window = exchange(packed, extra, coef)
    return analyse(background, stencil, frac, window)


def solution(mesh):
    return jax.shard_map(
        on_device,
        mesh=mesh,
        in_specs=(
            P(("lat", "lon"), None, None),
            P(("lat", "lon"), None),
            P(("lat", "lon"), None),
            P(("lat", "lon"), None),
            P(("lat", "lon"), None),
            P(("lat", "lon"), None),
            P(("lat", "lon")),
            P(("lat", "lon"), None),
            P("lat", "lon", None),
            P(None, "lat", "lon"),
            P(None, "lat", "lon"),
        ),
        out_specs=P("lat", "lon", None),
        check_vma=False,
    )
```

```python
import jax
import jax.numpy as jnp
from jax import lax
from jax.experimental import pallas as pl
from jax.experimental.pallas import tpu as pltpu
from jax.sharding import PartitionSpec as P

MEMBERS = 256
NOBS = 512
BAT = 32
TOP = 3
PTS = 8
ITERS = 6
HALF = 128
MESH = pl.DeviceIdType.MESH
F32 = jnp.float32
BF16 = jnp.bfloat16
COPIES = 64
GROUP = 4
CENTRE = MEMBERS - 1


def iota(shape, dim):
    return lax.broadcasted_iota(jnp.int32, shape, dim)


def dot(a, b):
    return jnp.dot(a, b, preferred_element_type=F32)


def dot_last(a, b):
    return lax.dot_general(a, b, (((1,), (1,)), ((), ())), preferred_element_type=F32)


def flip(x, z, dim):
    if dim == 0:
        return x + 1 - 2 * (x % 2), z
    if dim == 1:
        return 3 - x, z
    if dim == 2:
        return x, z + 1 - 2 * (z % 2)
    return x, 3 - z


def gray_bits(x, z):
    high_x, high_z = x // 2, z // 2
    low_x, low_z = (x % 2 + high_x) % 2, (z % 2 + high_z) % 2
    return (low_x, high_x, low_z, high_z)


def root_iteration(e_s, eb_s, z_s, scal, k):
    new = []
    for p in range(4):
        m, z = scal[p]
        f = 1.5 - 0.5 * m
        e = e_s[p]
        eb = eb_s[p]
        if k == 0:
            z_s[p] = -0.5 * e
        else:
            r = z_s[p]
            z_s[p] = f * r - 0.5 * (dot(r.astype(BF16), eb) + z * e)
        if k < ITERS - 1:
            g = m * f
            h = (f - 0.5 * m) * e - 0.5 * dot(eb, eb)
            e_new = f * h - 0.5 * (g * e + dot(h.astype(BF16), eb))
            e_s[p] = e_new
            eb_s[p] = e_new.astype(BF16)
        new.append((m * f * f, z * f))
    return new


def step_kernel(
    owner_h,
    points_h,
    count_h,
    len_h,
    weight_h,
    innov_h,
    taper_h,
    pert_h,
    back_h,
    stencil_h,
    frac_h,
    out_ref,
    pert,
    weight,
    innov,
    taper,
    owner_v,
    points_v,
    count_v,
    len_s,
    back,
    stencil,
    frac,
    wide_w,
    wide_i,
    source_v,
    source_s,
    coef,
    held,
    coef_n,
    coef_d,
    send3,
    recv3,
    send4,
    recv4,
    mine1,
    total,
    xheld,
    xsend3,
    xrecv3,
    xsend4,
    xrecv4,
    xmine1,
    xtotal,
    e_s,
    eb_s,
    z_s,
    window,
    lhs_s,
    xlhs_s,
    cells,
    mean_s,
    mixed,
    small_sems,
    pert_sems,
    first_send,
    first_recv,
    send_sems,
    recv_sems,
):
    lat, lon = lax.axis_index("lat"), lax.axis_index("lon")
    x, z = lon // 4, lon % 4
    odd = lat % 2
    lead = (odd, 1 - odd)

    def to(dim):
        hx, hz = flip(x, z, dim % 4)
        return (lat, hx * 4 + hz)

    east, west = (lat, (lon + 1) % 16), (lat, (lon + 15) % 16)
    outer, inner = ((lat + 7 + 2 * odd) % 8, lon), (lat + 1 - 2 * odd, lon)

    barrier = pltpu.get_barrier_semaphore()
    peers = [to(d) for d in range(4)] + [east, west, outer, inner]
    for peer in peers:
        pl.semaphore_signal(barrier, inc=1, device_id=peer, device_id_type=MESH)

    small = []
    for n, (src, dst) in enumerate(
        (
            (owner_h, owner_v),
            (points_h, points_v),
            (count_h, count_v),
            (taper_h, taper),
            (len_h, len_s),
            (weight_h, weight),
            (innov_h, innov),
            (stencil_h, stencil),
            (frac_h, frac),
            (back_h, back),
        )
    ):
        small.append(pltpu.make_async_copy(src, dst, small_sems.at[n]))
    for c in small[:7]:
        c.start()
    fetches = []
    for g in range(BAT // GROUP):
        rows = pl.ds(g * GROUP, GROUP)
        fetches.append(pltpu.make_async_copy(pert_h.at[rows], pert.at[rows], pert_sems.at[g]))
        fetches[g].start()
    for c in small[7:]:
        c.start()

    for c in small[:4]:
        c.wait()
    owner_row = owner_v[...]
    turned = jnp.broadcast_to(owner_row, (BAT, BAT)).T
    before = (turned == owner_row) & (iota((BAT, BAT), 0) < iota((BAT, BAT), 1))
    rank_row = jnp.sum(jnp.where(before, 1, 0), axis=0, keepdims=True)
    mine = gray_bits(x, z)
    theirs = gray_bits(owner_row // 4, owner_row % 4)
    rel_row = jnp.zeros((1, BAT), jnp.int32)
    for d in range(4):
        rel_row = rel_row + ((theirs[d] + mine[d]) % 2) * (1 << d)
    slots = iota((HALF, BAT), 0)
    slot_rows = jnp.broadcast_to(rel_row * 4 + rank_row, (BAT, BAT)).T
    fills = jnp.broadcast_to(slot_rows[:, 0:1], (BAT, HALF)) == iota((BAT, HALF), 1)
    source = jnp.sum(jnp.where(fills, iota((BAT, HALF), 0), 0), axis=0, keepdims=True)
    source_v[...] = jnp.broadcast_to(source, (PTS, HALF))
    table = pltpu.make_async_copy(source_v, source_s, small_sems.at[10])
    table.start()
    points, listed = points_v[...], taper[...].astype(F32)
    q = iota((PTS, BAT), 0)
    point = jnp.where(
        q < 4, (q // 2) * 4 + (q % 2) * 3, ((q - 4) // 2) * 4 + 1 + q % 2
    )
    weights = jnp.zeros((PTS, BAT), F32)
    for j in range(TOP):
        hit = (point == points[j : j + 1, :]) & (count_v[...] > j)
        weights = weights + jnp.where(hit, listed[j : j + 1, :], 0.0)
    spot = jnp.where(slots == owner_row * 4 + rank_row, 1.0, 0.0).astype(BF16)
    coef[...] = dot_last(weights.astype(BF16), spot)
    for c in small[4:7]:
        c.wait()
    wide_w[...] = weight[...].astype(F32)
    wide_i[...] = innov[...].astype(F32)
    table.wait()
    pl.semaphore_wait(barrier, len(peers))

    used = []

    def push(src, dst, peer):
        n = len(used)
        c = pltpu.make_async_remote_copy(
            src_ref=src,
            dst_ref=dst,
            send_sem=send_sems.at[n],
            recv_sem=recv_sems.at[n],
            device_id=peer,
            device_id_type=MESH,
        )
        c.start()
        used.append(c)
        return c

    def first_copy(k, at):
        return pltpu.make_async_remote_copy(
            src_ref=held.at[k, at + 8, :, 0],
            dst_ref=held.at[k, at, :, 1],
            send_sem=first_send.at[k, at],
            recv_sem=first_recv.at[k, at],
            device_id=to(k),
            device_id_type=MESH,
        )

    row, col = iota((HALF, HALF), 0), iota((HALF, HALF), 1)
    tail_row = iota((16, NOBS), 0)
    for c in fetches:
        c.wait()

    def one_owner(n, carry):
        rel = 15 - n
        bits = [(rel // (1 << d)) % 2 for d in range(4)]
        place = [
            bits[k] * 8 + bits[(k + 1) % 4] * 4 + bits[(k + 2) % 4] * 2 + bits[(k + 3) % 4]
            for k in range(4)
        ]
        kinds = []
        for s in range(4):
            b = jnp.minimum(jnp.maximum(source_s[0, rel * 4 + s], 0), BAT - 1)
            p = pert[b]
            live = iota((1, NOBS), 1) < len_s[0, b]
            w = jnp.where(live, wide_w[pl.ds(b, 1), :], 0.0)
            wi = w * wide_i[pl.ds(b, 1), :]
            high = wi.astype(BF16).astype(F32)
            tail = jnp.where(tail_row == 0, high, jnp.where(tail_row == 1, wi - high, 0.0))
            scaled = p.T * w.astype(BF16)
            acc = dot(jnp.concatenate([scaled, tail.astype(BF16)], axis=0), p)
            corner = acc[HALF:256, HALF:256]
            left = jnp.where(col >= row, acc[0:HALF, 0:HALF], corner)
            top = jnp.concatenate([left, acc[0:HALF, HALF:256]], axis=1).astype(BF16)
            for k in range(4):
                for rc in range(2):
                    at = 32 * k + 16 * rc
                    held[k, place[k], rc, 0, s] = top[at : at + 16, :]
            proj = acc[256:257, :] + acc[257:258, :]
            diagonal = jnp.sum(jnp.where(col == row, corner, 0.0), axis=0, keepdims=True)
            kinds += [diagonal, proj[:, 0:HALF], proj[:, HALF:256], jnp.zeros((1, HALF), F32)]
        xheld[place[0], 0] = jnp.concatenate(kinds, axis=0).astype(BF16)
        for k in range(4):

            @pl.when(bits[k] == 1)
            def _():
                first_copy(k, place[k] % 8).start()

        return carry

    cn = [push(coef, coef_n.at[k], to(k)) for k in range(4)]
    lax.fori_loop(0, 16, one_owner, 0)
    x1 = push(xheld.at[8:16, 0], xheld.at[0:8, 1], to(0))
    for k in range(4):
        cn[k].wait_recv()
    cd = [push(coef_n.at[k], coef_d.at[k], to(k + 1)) for k in range(4)]

    def sources(k):
        rows = [coef[...], coef_n[k], coef_n[(k + 1) % 4], coef_d[k]]
        return jnp.concatenate(rows, axis=0).astype(BF16)

    def served(k, pos):
        sx, sz = x, z
        if pos & 2:
            sx, sz = flip(sx, sz, (k + 2) % 4)
        if pos & 1:
            sx, sz = flip(sx, sz, (k + 3) % 4)
        return sx * 4 + sz

    def spread(k, pos, width, each):
        lane = iota((HALF, width), 1)
        pick = jnp.where(
            iota((HALF, width), 0) == served(k, pos) * 4 + (lane // each) % 4, 1.0, 0.0
        ).astype(BF16)
        every = dot(sources(k), pick)
        lane8 = iota((8, width), 1) // (4 * each)
        out = jnp.zeros((8, width), F32)
        for j in range(4):
            out = out + jnp.where(lane8 == j, every[8 * j : 8 * j + 8, :], 0.0)
        return out

    def expand(weights, rows, each):
        width = weights.shape[1]
        keep = iota((rows, width), 1) % each == iota((rows, width), 0)
        blocks = [
            jnp.where(keep, jnp.broadcast_to(weights[p : p + 1, :], (rows, width)), 0.0)
            for p in range(PTS)
        ]
        return jnp.concatenate(blocks, axis=0).astype(BF16)

    def merged(k, pos):
        lhs = lhs_s[k, pos]
        return [
            dot(lhs, held[k, pos, rc].reshape(256, 256)).reshape(PTS, 16, 256) for rc in range(2)
        ]

    def xmerged(pos):
        return dot(xlhs_s[pos][:, 0:64], xheld[pos].reshape(64, HALF))

    for k in range(4):
        cd[k].wait_recv()
    for pos in range(4):
        for k in range(4):
            lhs_s[k, pos] = expand(spread(k, pos, 256, 16), 16, 16)
        xlhs_s[pos] = expand(spread(0, pos, HALF, 4), 8, 4)

    s2a, s2b = [], []
    for k in range(4):
        for at in range(4, 8):
            first_copy(k, at).wait_recv()
        s2a.append(push(held.at[k, 6:8, :, 0:2], held.at[k, 2:4, :, 2:4], to(k + 1)))
    for k in range(4):
        s2b.append(push(held.at[k, 4:6, :, 0:2], held.at[k, 0:2, :, 2:4], to(k + 1)))
    x1.wait_recv()
    x2 = push(xheld.at[4:8, 0:2], xheld.at[0:4, 2:4], to(1))

    for c in small[7:]:
        c.wait()
    corner_id = (stencil[0] - (lat * 2 - 1)) * 6 + (stencil[1] - lon * 4 + 65) % 64
    fy, fx = frac[0], frac[1]
    corners = (
        (0, (1.0 - fy) * (1.0 - fx)),
        (6, fy * (1.0 - fx)),
        (1, (1.0 - fy) * fx),
        (7, fy * fx),
    )
    for t in range(4):
        turned = back[2 * t : 2 * t + 2].reshape(256, 256).T.astype(F32)
        mean = jnp.sum(turned, axis=0, keepdims=True) * (1.0 / MEMBERS)
        mean_s[t] = jnp.broadcast_to(mean, (8, 256))
        deviation = (turned - mean).astype(BF16).astype(F32)
        for j in range(24):
            value = jnp.zeros((8, HALF), F32)
            for add, share in corners:
                value = value + jnp.where(corner_id + add == j, share, 0.0)
            share = jnp.concatenate([value[2 * t : 2 * t + 1], value[2 * t + 1 : 2 * t + 2]], axis=1)
            cells[j, t] = (deviation * share).astype(BF16)

    for k in range(4):
        for at in range(4):
            first_copy(k, at).wait_recv()
    s3a, s3b = [], []
    for pos in (3, 2):
        for k in range(4):
            if pos == 3:
                s2a[k].wait_recv()
            for rc, value in enumerate(merged(k, pos)):
                send3[k, pos - 2, :, 16 * rc : 16 * rc + 16, :] = value.astype(BF16)
            if pos == 3:
                s3a.append(push(send3.at[k, 1], recv3.at[k, 1], to(k + 2)))
            else:
                for h in range(2):
                    span = pl.ds(4 * h, 4)
                    s3b.append(push(send3.at[k, 0, span], recv3.at[k, 0, span], to(k + 2)))
    x2.wait_recv()
    for pos in (3, 2):
        xsend3[pos - 2] = xmerged(pos).astype(BF16)
    x3 = push(xsend3, xrecv3, to(2))

    for pos in (1, 0):
        for k in range(4):
            if pos == 1:
                s2b[k].wait_recv()
            for rc, value in enumerate(merged(k, pos)):
                if pos == 1:
                    mine1[k, :, 16 * rc : 16 * rc + 16, :] = value
                else:
                    at = 32 * k + 16 * rc
                    total[:, at : at + 16, :] = value
    xmine1[...] = xmerged(1)
    xtotal[...] = xmerged(0)

    s4 = []

    def half4(k, h):
        span = pl.ds(4 * h, 4)
        return push(send4.at[k, span], recv4.at[k, span], to(k + 3))

    for k in range(4):
        s3a[k].wait_recv()
        send4[k] = (mine1[k] + recv3[k, 1].astype(F32)).astype(BF16)
        s4.append(half4(k, 0))
    x3.wait_recv()
    xsend4[...] = (xmine1[...] + xrecv3[1].astype(F32)).astype(BF16)
    x4 = push(xsend4, xrecv4, to(3))
    for k in range(4):
        s4.append(half4(k, 1))
    x4.wait_recv()
    xtotal[...] += xrecv3[0].astype(F32) + xrecv4[...].astype(F32)

    outside, inside, side = [], [], []

    def rim(a, slot, column):
        if a == 0:
            outside.append((column, push(window.at[slot], window.at[18 * (1 - odd) + column], outer)))
        else:
            inside.append((column, push(window.at[slot], window.at[18 * odd + column], inner)))

    def corners_on():
        for a in range(2):
            for j in range(2):
                side[2 * a + j].wait_recv()
                column = 5 - 5 * j
                rim(a, (lead[a] + 1) * 6 + column, column)

    eye = jnp.where(row == col, float(CENTRE), 0.0)
    for g in range(2):
        scal, scales = [], []
        for k in range(4):
            s3b[2 * k + g].wait_recv()
            s4[4 * g + k].wait_recv()
        for i in range(4):
            p = 4 * g + i
            for k in range(4):
                total[p, 32 * k : 32 * k + 32, :] += recv3[k, 0, p].astype(F32) + recv4[
                    k, p
                ].astype(F32)
            left, right = total[p, :, 0:HALF], total[p, :, HALF:256]
            turned = left.T
            a = jnp.where(col >= row, left, turned) + eye
            c = jnp.where(col < row, left, turned)
            c = jnp.where(col == row, xtotal[8 * p : 8 * p + 1, :], c) + eye
            square = jnp.sum(a * a + c * c + 2.0 * (right * right), keepdims=True)
            trace = jnp.sum(jnp.where(row == col, a + c, 0.0), keepdims=True)
            scale = jnp.sqrt(square)
            inverse = 1.0 / scale
            mean = trace * (1.0 / MEMBERS)
            off = jnp.where(row == col, mean, 0.0)
            a, c, b = (a - off) * inverse, (c - off) * inverse, right * inverse
            e_s[i] = jnp.concatenate(
                [jnp.concatenate([a, b], axis=1), jnp.concatenate([b.T, c], axis=1)], axis=0
            )
            eb_s[i] = e_s[i].astype(BF16)
            scal.append((mean * inverse, jnp.ones((1, 1), F32)))
            scales.append(scale)
        for k in range(ITERS):
            scal = root_iteration(e_s, eb_s, z_s, scal, k)
            if g == 1 and k == 3:
                corners_on()
        big = iota((256, 256), 0) == iota((256, 256), 1)
        tail16 = iota((16, 256), 0)
        for a in range(2):
            for j in range(2):
                i = 2 * lead[a] + j
                flag = jnp.full((1, 1), lead[a], jnp.int32) == 1
                zd = jnp.where(flag, scal[2 + j][1], scal[j][1])
                scale = jnp.where(flag, scales[2 + j], scales[j])
                r = z_s[i]
                high = r.astype(BF16)
                low = (r - high.astype(F32)).astype(BF16)

                def apply(v):
                    vh = v.astype(BF16).astype(F32)
                    both = jnp.where(tail16 == 0, vh, jnp.where(tail16 == 1, v - vh, 0.0)).astype(
                        BF16
                    )
                    w = dot(both, high) + dot(both, low)
                    return zd * v + w[0:1, :] + w[1:2, :]

                kinds = xtotal[pl.ds(pl.multiple_of(8 * (4 * g + i), 8), 8), :]
                shift = jnp.concatenate([kinds[1:2], kinds[2:3]], axis=1)
                mw = apply(apply(shift)) / scale
                amp = jnp.sqrt(float(CENTRE) / scale)
                full = amp * (r + jnp.where(big, zd, 0.0)) + mw
                column = 1 + 3 * j if g == 0 else 2 + j
                slot = (lead[a] + 1) * 6 + column
                window[slot] = full.astype(BF16)
                if g == 0:
                    across = window.at[(lead[a] + 1) * 6 + 5 - 5 * j]
                    side.append(push(window.at[slot], across, west if j == 0 else east))
                rim(a, slot, column)

    def gather(slots, start=False):
        for t in range(4):
            part = dot(window[slots[0]], cells[slots[0], t])
            for n in slots[1:]:
                part = part + dot(window[n], cells[n, t])
            mixed[t] = part if start else mixed[t] + part

    gather([6 * r + c for r in (1, 2) for c in range(6)], start=True)
    for column, c in inside:
        c.wait_recv()
    gather([18 * (1 - odd) + column for column in range(6)])
    for column, c in outside:
        if column not in (2, 3):
            c.wait_recv()
    gather([18 * odd + column for column in (0, 1, 4, 5)])
    for column, c in outside:
        if column in (2, 3):
            c.wait_recv()
    for t in range(4):
        far = 18 * odd
        part = mixed[t] + dot(window[far + 2], cells[far + 2, t]) + dot(
            window[far + 3], cells[far + 3, t]
        )
        whole = (part + mean_s[t][0:1, :]).astype(BF16)
        out_ref[2 * t : 2 * t + 2] = whole.T.reshape(2, HALF, 256)
    for k in range(4):
        for at in range(8):
            first_copy(k, at).wait_send()
    for c in used:
        c.wait_send()


def step(args):
    hbm = pl.BlockSpec(memory_space=pl.ANY)
    i32 = jnp.int32
    vm = pltpu.VMEM
    return pl.pallas_call(
        step_kernel,
        out_shape=jax.ShapeDtypeStruct((8, HALF, 256), BF16),
        in_specs=[hbm] * len(args),
        out_specs=pl.BlockSpec(memory_space=pltpu.VMEM),
        scratch_shapes=[
            vm((BAT, NOBS, MEMBERS), BF16),
            vm((BAT, NOBS), BF16),
            vm((BAT, NOBS), BF16),
            vm((TOP, BAT), BF16),
            vm((1, BAT), i32),
            vm((TOP, BAT), i32),
            vm((1, BAT), i32),
            pltpu.SMEM((1, BAT), i32),
            vm((8, HALF, 256), BF16),
            vm((2, 8, HALF), i32),
            vm((2, 8, HALF), F32),
            vm((BAT, NOBS), F32),
            vm((BAT, NOBS), F32),
            vm((PTS, HALF), i32),
            pltpu.SMEM((PTS, HALF), i32),
            vm((PTS, HALF), F32),
            vm((4, 16, 2, 4, 4, 16, 256), BF16),
            vm((4, PTS, HALF), F32),
            vm((4, PTS, HALF), F32),
            vm((4, 2, PTS, 32, 256), BF16),
            vm((4, 2, PTS, 32, 256), BF16),
            vm((4, PTS, 32, 256), BF16),
            vm((4, PTS, 32, 256), BF16),
            vm((4, PTS, 32, 256), F32),
            vm((PTS, HALF, 256), F32),
            vm((16, 4, 16, HALF), BF16),
            vm((2, 64, HALF), BF16),
            vm((2, 64, HALF), BF16),
            vm((64, HALF), BF16),
            vm((64, HALF), BF16),
            vm((64, HALF), F32),
            vm((64, HALF), F32),
            vm((4, 256, 256), F32),
            vm((4, 256, 256), BF16),
            vm((4, 256, 256), F32),
            vm((24, 256, 256), BF16),
            vm((4, 4, HALF, 256), BF16),
            vm((4, 64, HALF), BF16),
            vm((24, 4, 256, 256), BF16),
            vm((4, 8, 256), F32),
            vm((4, 256, 256), F32),
            pltpu.SemaphoreType.DMA((11,)),
            pltpu.SemaphoreType.DMA((BAT // GROUP,)),
            pltpu.SemaphoreType.DMA((4, 8)),
            pltpu.SemaphoreType.DMA((4, 8)),
            pltpu.SemaphoreType.DMA((COPIES,)),
            pltpu.SemaphoreType.DMA((COPIES,)),
        ],
        compiler_params=pltpu.CompilerParams(
            collective_id=0, has_side_effects=True, vmem_limit_bytes=67043328
        ),
        name="step",
    )(*args)


def on_device(
    obs_pert,
    obs_weight,
    innovation,
    batch_len,
    batch_owner,
    batch_points,
    batch_count,
    batch_taper,
    background,
    stencil,
    frac,
):
    return step(
        (
            batch_owner.T,
            batch_points.T,
            batch_count.reshape(1, BAT),
            batch_len,
            obs_weight,
            innovation,
            batch_taper.T,
            obs_pert,
            background,
            stencil,
            frac,
        )
    )


def solution(mesh):
    return jax.shard_map(
        on_device,
        mesh=mesh,
        in_specs=(
            P(("lat", "lon"), None, None),
            P(("lat", "lon"), None),
            P(("lat", "lon"), None),
            P(("lat", "lon"), None),
            P(("lat", "lon"), None),
            P(("lat", "lon"), None),
            P(("lat", "lon")),
            P(("lat", "lon"), None),
            P("lat", "lon", None),
            P(None, "lat", "lon"),
            P(None, "lat", "lon"),
        ),
        out_specs=P("lat", "lon", None),
        check_vma=False,
    )
```

```python
import jax
import jax.numpy as jnp
from jax import lax
from jax.experimental import pallas as pl
from jax.experimental.pallas import tpu as pltpu
from jax.sharding import PartitionSpec as P

MEMBERS = 256
NOBS = 512
BAT = 32
TOP = 3
PTS = 8
ITERS = 6
HALF = 128
MESH = pl.DeviceIdType.MESH
F32 = jnp.float32
BF16 = jnp.bfloat16
COPIES = 64
GROUP = 4
CENTRE = MEMBERS - 1


def iota(shape, dim):
    return lax.broadcasted_iota(jnp.int32, shape, dim)


def dot(a, b):
    return jnp.dot(a, b, preferred_element_type=F32)


def dot_last(a, b):
    return lax.dot_general(a, b, (((1,), (1,)), ((), ())), preferred_element_type=F32)


def flip(x, z, dim):
    if dim == 0:
        return x + 1 - 2 * (x % 2), z
    if dim == 1:
        return 3 - x, z
    if dim == 2:
        return x, z + 1 - 2 * (z % 2)
    return x, 3 - z


def gray_bits(x, z):
    high_x, high_z = x // 2, z // 2
    low_x, low_z = (x % 2 + high_x) % 2, (z % 2 + high_z) % 2
    return (low_x, high_x, low_z, high_z)


def root_iteration(phi_s, low_s, xi_s, scal, k):
    four, last = range(4), k == ITERS - 1
    f = [1.5 - 0.5 * scal[p][0] for p in four]
    m_new = [scal[p][0] * f[p] * f[p] for p in four]
    back = [-0.5 * scal[p][0] / f[p] for p in four]
    if not last:
        square = [dot(low_s[p], low_s[p]) for p in four]
    if k:
        grown = [dot(xi_s[p].astype(BF16), low_s[p]) for p in four]
    if not last:
        both = [((2.0 + back[p]) * phi_s[p] + square[p]).astype(BF16) for p in four]
        cubic = [dot(both[p], low_s[p]) for p in four]
    for p in four:
        xi_s[p] = (xi_s[p] + phi_s[p]) + grown[p] if k else phi_s[p]
    if not last:
        for p in four:
            ratio = f[p] * f[p] * f[p] / (1.5 - 0.5 * m_new[p])
            phi_new = (ratio * (1.0 + 2.0 * back[p])) * phi_s[p] + ratio * cubic[p]
            phi_s[p] = phi_new
            low_s[p] = phi_new.astype(BF16)
    return [(m_new[p], scal[p][1] * f[p]) for p in four]


def step_kernel(
    owner_h,
    points_h,
    count_h,
    len_h,
    weight_h,
    innov_h,
    taper_h,
    pert_h,
    back_h,
    stencil_h,
    frac_h,
    out_ref,
    pert,
    weight,
    innov,
    taper,
    owner_v,
    points_v,
    count_v,
    len_s,
    back,
    stencil,
    frac,
    wide_w,
    wide_i,
    source_v,
    source_s,
    coef,
    held,
    coef_n,
    coef_d,
    send3,
    recv3,
    send4,
    recv4,
    mine1,
    total,
    xheld,
    xsend3,
    xrecv3,
    xsend4,
    xrecv4,
    xmine1,
    xtotal,
    e_s,
    eb_s,
    z_s,
    window,
    rims,
    lhs_s,
    xlhs_s,
    cells,
    mean_s,
    mixed,
    done,
    small_sems,
    pert_sems,
    first_send,
    first_recv,
    send_sems,
    recv_sems,
):
    lat, lon = lax.axis_index("lat"), lax.axis_index("lon")
    x, z = lon // 4, lon % 4
    odd = lat % 2
    lead = (odd, 1 - odd)

    def to(dim):
        hx, hz = flip(x, z, dim % 4)
        return (lat, hx * 4 + hz)

    east, west = (lat, (lon + 1) % 16), (lat, (lon + 15) % 16)
    outer, inner = ((lat + 7 + 2 * odd) % 8, lon), (lat + 1 - 2 * odd, lon)

    barrier = pltpu.get_barrier_semaphore()
    peers = [to(d) for d in range(4)] + [east, west, outer, inner]
    for peer in peers:
        pl.semaphore_signal(barrier, inc=1, device_id=peer, device_id_type=MESH)

    small = []
    for n, (src, dst) in enumerate(
        (
            (owner_h, owner_v),
            (points_h, points_v),
            (count_h, count_v),
            (taper_h, taper),
            (len_h, len_s),
            (weight_h, weight),
            (innov_h, innov),
            (stencil_h, stencil),
            (frac_h, frac),
            (back_h, back),
        )
    ):
        small.append(pltpu.make_async_copy(src, dst, small_sems.at[n]))
    for c in small[:7]:
        c.start()
    fetches = []
    for g in range(BAT // GROUP):
        rows = pl.ds(g * GROUP, GROUP)
        fetches.append(pltpu.make_async_copy(pert_h.at[rows], pert.at[rows], pert_sems.at[g]))
        fetches[g].start()
    for c in small[7:]:
        c.start()

    for c in small[:4]:
        c.wait()
    owner_row = owner_v[...]
    turned = jnp.broadcast_to(owner_row, (BAT, BAT)).T
    before = (turned == owner_row) & (iota((BAT, BAT), 0) < iota((BAT, BAT), 1))
    rank_row = jnp.sum(jnp.where(before, 1, 0), axis=0, keepdims=True)
    mine = gray_bits(x, z)
    theirs = gray_bits(owner_row // 4, owner_row % 4)
    rel_row = jnp.zeros((1, BAT), jnp.int32)
    for d in range(4):
        rel_row = rel_row + ((theirs[d] + mine[d]) % 2) * (1 << d)
    slots = iota((HALF, BAT), 0)
    slot_rows = jnp.broadcast_to(rel_row * 4 + rank_row, (BAT, BAT)).T
    fills = jnp.broadcast_to(slot_rows[:, 0:1], (BAT, HALF)) == iota((BAT, HALF), 1)
    source = jnp.sum(jnp.where(fills, iota((BAT, HALF), 0), 0), axis=0, keepdims=True)
    source_v[...] = jnp.broadcast_to(source, (PTS, HALF))
    table = pltpu.make_async_copy(source_v, source_s, small_sems.at[10])
    table.start()
    points, listed = points_v[...], taper[...].astype(F32)
    q = iota((PTS, BAT), 0)
    point = jnp.where(
        q < 4, (q // 2) * 4 + (q % 2) * 3, ((q - 4) // 2) * 4 + 1 + q % 2
    )
    weights = jnp.zeros((PTS, BAT), F32)
    for j in range(TOP):
        hit = (point == points[j : j + 1, :]) & (count_v[...] > j)
        weights = weights + jnp.where(hit, listed[j : j + 1, :], 0.0)
    spot = jnp.where(slots == owner_row * 4 + rank_row, 1.0, 0.0).astype(BF16)
    coef[...] = dot_last(weights.astype(BF16), spot)
    for c in small[4:7]:
        c.wait()
    wide_w[...] = weight[...].astype(F32)
    wide_i[...] = innov[...].astype(F32)
    table.wait()
    pl.semaphore_wait(barrier, len(peers))

    used = []

    def push(src, dst, peer):
        n = len(used)
        c = pltpu.make_async_remote_copy(
            src_ref=src,
            dst_ref=dst,
            send_sem=send_sems.at[n],
            recv_sem=recv_sems.at[n],
            device_id=peer,
            device_id_type=MESH,
        )
        c.start()
        used.append(c)
        return c

    def first_copy(k, at):
        return pltpu.make_async_remote_copy(
            src_ref=held.at[k, at + 8, :, 0],
            dst_ref=held.at[k, at, :, 1],
            send_sem=first_send.at[k, at],
            recv_sem=first_recv.at[k, at],
            device_id=to(k),
            device_id_type=MESH,
        )

    row, col = iota((HALF, HALF), 0), iota((HALF, HALF), 1)
    tail_row = iota((16, NOBS), 0)
    for c in fetches:
        c.wait()

    def one_owner(n, carry):
        rel = 15 - n
        bits = [(rel // (1 << d)) % 2 for d in range(4)]
        place = [
            bits[k] * 8 + bits[(k + 1) % 4] * 4 + bits[(k + 2) % 4] * 2 + bits[(k + 3) % 4]
            for k in range(4)
        ]
        kinds = []
        for s in range(4):
            b = jnp.minimum(jnp.maximum(source_s[0, rel * 4 + s], 0), BAT - 1)
            p = pert[b]
            live = iota((1, NOBS), 1) < len_s[0, b]
            w = jnp.where(live, wide_w[pl.ds(b, 1), :], 0.0)
            wi = w * wide_i[pl.ds(b, 1), :]
            high = wi.astype(BF16).astype(F32)
            tail = jnp.where(tail_row == 0, high, jnp.where(tail_row == 1, wi - high, 0.0))
            scaled = p.T * w.astype(BF16)
            acc = dot(jnp.concatenate([scaled, tail.astype(BF16)], axis=0), p)
            corner = acc[HALF:256, HALF:256]
            left = jnp.where(col >= row, acc[0:HALF, 0:HALF], corner)
            top = jnp.concatenate([left, acc[0:HALF, HALF:256]], axis=1).astype(BF16)
            for k in range(4):
                for rc in range(2):
                    at = 32 * k + 16 * rc
                    held[k, place[k], rc, 0, s] = top[at : at + 16, :]
            proj = acc[256:257, :] + acc[257:258, :]
            diagonal = jnp.sum(jnp.where(col == row, corner, 0.0), axis=0, keepdims=True)
            kinds += [diagonal, proj[:, 0:HALF], proj[:, HALF:256], jnp.zeros((1, HALF), F32)]
        xheld[place[0], 0] = jnp.concatenate(kinds, axis=0).astype(BF16)
        for k in range(4):

            @pl.when(bits[k] == 1)
            def _():
                first_copy(k, place[k] % 8).start()

        return carry

    cn = [push(coef, coef_n.at[k], to(k)) for k in range(4)]
    lax.fori_loop(0, 16, one_owner, 0)
    x1 = push(xheld.at[8:16, 0], xheld.at[0:8, 1], to(0))
    for k in range(4):
        cn[k].wait_recv()
    cd = [push(coef_n.at[k], coef_d.at[k], to(k + 1)) for k in range(4)]

    def sources(k):
        rows = [coef[...], coef_n[k], coef_n[(k + 1) % 4], coef_d[k]]
        return jnp.concatenate(rows, axis=0).astype(BF16)

    def served(k, pos):
        sx, sz = x, z
        if pos & 2:
            sx, sz = flip(sx, sz, (k + 2) % 4)
        if pos & 1:
            sx, sz = flip(sx, sz, (k + 3) % 4)
        return sx * 4 + sz

    def spread(k, pos, width, each):
        lane = iota((HALF, width), 1)
        pick = jnp.where(
            iota((HALF, width), 0) == served(k, pos) * 4 + (lane // each) % 4, 1.0, 0.0
        ).astype(BF16)
        every = dot(sources(k), pick)
        lane8 = iota((8, width), 1) // (4 * each)
        out = jnp.zeros((8, width), F32)
        for j in range(4):
            out = out + jnp.where(lane8 == j, every[8 * j : 8 * j + 8, :], 0.0)
        return out

    def expand(weights, rows, each):
        width = weights.shape[1]
        keep = iota((rows, width), 1) % each == iota((rows, width), 0)
        blocks = [
            jnp.where(keep, jnp.broadcast_to(weights[p : p + 1, :], (rows, width)), 0.0)
            for p in range(PTS)
        ]
        return jnp.concatenate(blocks, axis=0).astype(BF16)

    def xmerged(pos):
        return dot(xlhs_s[pos][:, 0:64], xheld[pos].reshape(64, HALF))

    for k in range(4):
        cd[k].wait_recv()
    for pos in range(4):
        for k in range(4):
            lhs_s[k, pos] = expand(spread(k, pos, 256, 16), 16, 16)
        xlhs_s[pos] = expand(spread(0, pos, HALF, 4), 8, 4)

    s2a, s2b = [], []
    for k in range(4):
        for at in range(4, 8):
            first_copy(k, at).wait_recv()
        s2a.append(push(held.at[k, 6:8, :, 0:2], held.at[k, 2:4, :, 2:4], to(k + 1)))
    for k in range(4):
        s2b.append(push(held.at[k, 4:6, :, 0:2], held.at[k, 0:2, :, 2:4], to(k + 1)))
    x1.wait_recv()
    x2 = push(xheld.at[4:8, 0:2], xheld.at[0:4, 2:4], to(1))

    for c in small[7:]:
        c.wait()
    corner_id = (stencil[0] - (lat * 2 - 1)) * 6 + (stencil[1] - lon * 4 + 65) % 64
    fy, fx = frac[0], frac[1]
    corners = (
        (0, (1.0 - fy) * (1.0 - fx)),
        (6, fy * (1.0 - fx)),
        (1, (1.0 - fy) * fx),
        (7, fy * fx),
    )
    for t in range(4):
        turned = back[2 * t : 2 * t + 2].reshape(256, 256).T.astype(F32)
        mean = jnp.sum(turned, axis=0, keepdims=True) * (1.0 / MEMBERS)
        mean_s[t] = jnp.broadcast_to(mean, (8, 256))
        deviation = (turned - mean).astype(BF16).astype(F32)
        for j in range(24):
            value = jnp.zeros((8, HALF), F32)
            for add, share in corners:
                value = value + jnp.where(corner_id + add == j, share, 0.0)
            share = jnp.concatenate([value[2 * t : 2 * t + 1], value[2 * t + 1 : 2 * t + 2]], axis=1)
            cells[j, t] = (deviation * share).astype(BF16)

    for k in range(4):
        for at in range(4):
            first_copy(k, at).wait_recv()

    def merge(k, pos, g):
        lhs = lhs_s[k, pos, 64 * g : 64 * g + 64, :]
        return [dot(lhs, held[k, pos, rc].reshape(256, 256)).reshape(4, 16, 256) for rc in range(2)]

    def send_on(pos, g):
        for k in range(4):
            if (pos, g) == (3, 0):
                s2a[k].wait_recv()
            span = slice(4 * g, 4 * g + 4)
            for rc, value in enumerate(merge(k, pos, g)):
                send3[k, pos - 2, span, 16 * rc : 16 * rc + 16, :] = value.astype(BF16)
            s3[pos, g, k] = push(send3.at[k, pos - 2, span], recv3.at[k, pos - 2, span], to(k + 2))

    def keep_own(g):
        for k in range(4):
            if g == 0:
                s2b[k].wait_recv()
            span = slice(4 * g, 4 * g + 4)
            for rc, value in enumerate(merge(k, 1, g)):
                mine1[k, span, 16 * rc : 16 * rc + 16, :] = value
            for rc, value in enumerate(merge(k, 0, g)):
                at = 32 * k + 16 * rc
                total[span, at : at + 16, :] = value

    def last_step(g):
        for k in range(4):
            s3[3, g, k].wait_recv()
            span = slice(4 * g, 4 * g + 4)
            send4[k, span] = (mine1[k, span] + recv3[k, 1, span].astype(F32)).astype(BF16)
            s4[g, k] = push(send4.at[k, span], recv4.at[k, span], to(k + 3))

    s3, s4 = {}, {}
    send_on(3, 0)
    send_on(2, 0)
    x2.wait_recv()
    for pos in (3, 2):
        xsend3[pos - 2] = xmerged(pos).astype(BF16)
    x3 = push(xsend3, xrecv3, to(2))
    send_on(3, 1)
    keep_own(0)
    xmine1[...] = xmerged(1)
    xtotal[...] = xmerged(0)
    last_step(0)
    x3.wait_recv()
    xsend4[...] = (xmine1[...] + xrecv3[1].astype(F32)).astype(BF16)
    x4 = push(xsend4, xrecv4, to(3))
    send_on(2, 1)
    keep_own(1)
    for k in range(4):
        for at in range(8):
            first_copy(k, at).wait_send()
    early = 18
    for c in used[:early]:
        c.wait_send()
    last_step(1)
    late = len(used)
    x4.wait_recv()
    xtotal[...] += xrecv3[0].astype(F32) + xrecv4[...].astype(F32)

    outside, inside, side = [], [], []

    def rim(a, slot, column):
        if a == 0:
            outside.append((column, push(rims.at[slot], rims.at[18 * (1 - odd) + column], outer)))
        else:
            inside.append((column, push(rims.at[slot], rims.at[18 * odd + column], inner)))

    def unfold(n):
        fold = rims[n, 0:HALF, 0:HALF].astype(F32)
        right = rims[n, 0:HALF, HALF:256]
        turned = fold.T
        a = jnp.where(col >= row, fold, turned)
        c = jnp.where(col < row, fold, turned)
        last = rims[n, HALF:144, :]
        c = jnp.where(col == row, last[:, 0:HALF].astype(F32)[2:3, :], c)
        window[n, 0:HALF, :] = jnp.concatenate([a.astype(BF16), right], axis=1)
        window[n, HALF:256, :] = jnp.concatenate([right.T, c.astype(BF16)], axis=1)
        window[n, 256:272, :] = last

    def corners_on(a):
        for j in range(2):
            side[2 * a + j].wait_recv()
            column = 5 - 5 * j
            rim(a, (lead[a] + 1) * 6 + column, column)
        for column in (0, 5):
            unfold((lead[a] + 1) * 6 + column)

    def gather(slots, start=False):
        for t in range(4):
            part = dot(window[slots[0]], cells[slots[0], t])
            for n in slots[1:]:
                part = part + dot(window[n], cells[n, t])
            mixed[t] = part if start else mixed[t] + part

    eye = jnp.where(row == col, float(CENTRE), 0.0)
    for g in range(2):
        scal, scales = [], []
        for k in range(4):
            s3[2, g, k].wait_recv()
            s4[g, k].wait_recv()
        for i in range(4):
            p = 4 * g + i
            for k in range(4):
                total[p, 32 * k : 32 * k + 32, :] += recv3[k, 0, p].astype(F32) + recv4[
                    k, p
                ].astype(F32)
            left, right = total[p, :, 0:HALF], total[p, :, HALF:256]
            turned = left.T
            a = jnp.where(col >= row, left, turned) + eye
            c = jnp.where(col < row, left, turned)
            c = jnp.where(col == row, xtotal[8 * p : 8 * p + 1, :], c) + eye
            square = jnp.sum(a * a + c * c + 2.0 * (right * right), keepdims=True)
            trace = jnp.sum(jnp.where(row == col, a + c, 0.0), keepdims=True)
            scale = jnp.sqrt(square)
            inverse = 1.0 / scale
            mean = trace * (1.0 / MEMBERS)
            off = jnp.where(row == col, mean, 0.0)
            slope = -0.5 * inverse / (1.5 - 0.5 * mean * inverse)
            a, c, b = (a - off) * slope, (c - off) * slope, right * slope
            e_s[i] = jnp.concatenate(
                [jnp.concatenate([a, b], axis=1), jnp.concatenate([b.T, c], axis=1)], axis=0
            )
            eb_s[i] = e_s[i].astype(BF16)
            scal.append((mean * inverse, jnp.ones((1, 1), F32)))
            scales.append(scale)
        for k in range(ITERS):
            scal = root_iteration(e_s, eb_s, z_s, scal, k)
            if g == 1 and k in (2, 3):
                corners_on(k - 2)
            if g == 1 and k == 3:
                for c in used[early:late]:
                    c.wait_send()
                gather([6 * r + c for r in (1, 2) for c in (0, 1, 4, 5)], start=True)
        big = iota((256, 256), 0) == iota((256, 256), 1)
        tail16 = iota((16, 256), 0)
        turns = []
        for a in range(2):
            for j in range(2):
                i = 2 * lead[a] + j
                flag = jnp.full((1, 1), lead[a], jnp.int32) == 1
                zd = jnp.where(flag, scal[2 + j][1], scal[j][1])
                scale = jnp.where(flag, scales[2 + j], scales[j])
                kinds = xtotal[pl.ds(pl.multiple_of(8 * (4 * g + i), 8), 8), :]
                shift = jnp.concatenate([kinds[1:2], kinds[2:3]], axis=1)
                turns.append([a, j, i, zd, scale, shift])
        for again in range(2):
            moved = []
            for a, j, i, zd, scale, v in turns:
                r = z_s[i]
                high = r.astype(BF16)
                low = (r - high.astype(F32)).astype(BF16)
                vh = v.astype(BF16).astype(F32)
                both = jnp.where(tail16 == 0, vh, jnp.where(tail16 == 1, v - vh, 0.0)).astype(BF16)
                moved.append(dot(both, high) + dot(both, low))
            for n, w in enumerate(moved):
                turns[n][5] = turns[n][3] * (turns[n][5] + w[0:1, :] + w[1:2, :])
        for a, j, i, zd, scale, v in turns:
            mw = v / scale
            amp = jnp.sqrt(float(CENTRE) / scale)
            whole = (amp * zd) * (z_s[i] + jnp.where(big, 1.0, 0.0))
            column = 1 + 3 * j if g == 0 else 2 + j
            slot = (lead[a] + 1) * 6 + column
            window[slot, 0:256, :] = whole.astype(BF16)
            corner = whole[HALF:256, HALF:256]
            fold = jnp.where(col >= row, whole[0:HALF, 0:HALF], corner)
            rims[slot, 0:HALF, :] = jnp.concatenate([fold, whole[0:HALF, HALF:256]], axis=1).astype(
                BF16
            )
            diagonal = jnp.sum(jnp.where(col == row, corner, 0.0), axis=0, keepdims=True)
            diagonal = jnp.concatenate([diagonal, jnp.zeros((1, HALF), F32)], axis=1)
            high = mw.astype(BF16).astype(F32)
            last = jnp.where(tail16 == 2, diagonal, 0.0)
            last = jnp.where(tail16 == 0, high, jnp.where(tail16 == 1, mw - high, last)).astype(BF16)
            rims[slot, HALF:144, :] = last
            window[slot, 256:272, :] = last
            if g == 0:
                across = rims.at[(lead[a] + 1) * 6 + 5 - 5 * j]
                side.append(push(rims.at[slot], across, west if j == 0 else east))
            rim(a, slot, column)

    gather([6 * r + c for r in (1, 2) for c in (2, 3)])
    for column, c in inside:
        c.wait_recv()
    near, far = 18 * (1 - odd), 18 * odd
    for column in range(6):
        unfold(near + column)
    gather([near + column for column in range(6)])
    for column, c in outside:
        if column not in (2, 3):
            c.wait_recv()
    for column in (0, 1, 4, 5):
        unfold(far + column)
    gather([far + column for column in (0, 1, 4, 5)])
    for column, c in outside:
        if column in (2, 3):
            c.wait_recv()
    for column in (2, 3):
        unfold(far + column)
    outs = []
    for t in range(4):
        part = mixed[t] + (
            dot(window[far + 2], cells[far + 2, t]) + dot(window[far + 3], cells[far + 3, t])
        )
        shared = part[256:257, :] + part[257:258, :] + mean_s[t][0:1, :]
        whole = (part[0:256, :] + shared).astype(BF16)
        done[2 * t : 2 * t + 2] = whole.T.reshape(2, HALF, 256)
        span = pl.ds(2 * t, 2)
        outs.append(pltpu.make_async_copy(done.at[span], out_ref.at[span], small_sems.at[t]))
        outs[t].start()
    for c in used[late:]:
        c.wait_send()
    for c in outs:
        c.wait()


def step(args):
    hbm = pl.BlockSpec(memory_space=pl.ANY)
    i32 = jnp.int32
    vm = pltpu.VMEM
    return pl.pallas_call(
        step_kernel,
        out_shape=jax.ShapeDtypeStruct((8, HALF, 256), BF16),
        in_specs=[hbm] * len(args),
        out_specs=hbm,
        scratch_shapes=[
            vm((BAT, NOBS, MEMBERS), BF16),
            vm((BAT, NOBS), BF16),
            vm((BAT, NOBS), BF16),
            vm((TOP, BAT), BF16),
            vm((1, BAT), i32),
            vm((TOP, BAT), i32),
            vm((1, BAT), i32),
            pltpu.SMEM((1, BAT), i32),
            vm((8, HALF, 256), BF16),
            vm((2, 8, HALF), i32),
            vm((2, 8, HALF), F32),
            vm((BAT, NOBS), F32),
            vm((BAT, NOBS), F32),
            vm((PTS, HALF), i32),
            pltpu.SMEM((PTS, HALF), i32),
            vm((PTS, HALF), F32),
            vm((4, 16, 2, 4, 4, 16, 256), BF16),
            vm((4, PTS, HALF), F32),
            vm((4, PTS, HALF), F32),
            vm((4, 2, PTS, 32, 256), BF16),
            vm((4, 2, PTS, 32, 256), BF16),
            vm((4, PTS, 32, 256), BF16),
            vm((4, PTS, 32, 256), BF16),
            vm((4, PTS, 32, 256), F32),
            vm((PTS, HALF, 256), F32),
            vm((16, 4, 16, HALF), BF16),
            vm((2, 64, HALF), BF16),
            vm((2, 64, HALF), BF16),
            vm((64, HALF), BF16),
            vm((64, HALF), BF16),
            vm((64, HALF), F32),
            vm((64, HALF), F32),
            vm((4, 256, 256), F32),
            vm((4, 256, 256), BF16),
            vm((4, 256, 256), F32),
            vm((24, 272, 256), BF16),
            vm((24, 144, 256), BF16),
            vm((4, 4, HALF, 256), BF16),
            vm((4, 64, HALF), BF16),
            vm((24, 4, 256, 256), BF16),
            vm((4, 8, 256), F32),
            vm((4, 272, 256), F32),
            vm((8, HALF, 256), BF16),
            pltpu.SemaphoreType.DMA((11,)),
            pltpu.SemaphoreType.DMA((BAT // GROUP,)),
            pltpu.SemaphoreType.DMA((4, 8)),
            pltpu.SemaphoreType.DMA((4, 8)),
            pltpu.SemaphoreType.DMA((COPIES,)),
            pltpu.SemaphoreType.DMA((COPIES,)),
        ],
        compiler_params=pltpu.CompilerParams(
            collective_id=0, has_side_effects=True, vmem_limit_bytes=67043328
        ),
        name="step",
    )(*args)


def on_device(
    obs_pert,
    obs_weight,
    innovation,
    batch_len,
    batch_owner,
    batch_points,
    batch_count,
    batch_taper,
    background,
    stencil,
    frac,
):
    return step(
        (
            batch_owner.T,
            batch_points.T,
            batch_count.reshape(1, BAT),
            batch_len,
            obs_weight,
            innovation,
            batch_taper.T,
            obs_pert,
            background,
            stencil,
            frac,
        )
    )


def solution(mesh):
    return jax.shard_map(
        on_device,
        mesh=mesh,
        in_specs=(
            P(("lat", "lon"), None, None),
            P(("lat", "lon"), None),
            P(("lat", "lon"), None),
            P(("lat", "lon"), None),
            P(("lat", "lon"), None),
            P(("lat", "lon"), None),
            P(("lat", "lon")),
            P(("lat", "lon"), None),
            P("lat", "lon", None),
            P(None, "lat", "lon"),
            P(None, "lat", "lon"),
        ),
        out_specs=P("lat", "lon", None),
        check_vma=False,
    )
```

```python
import jax
import jax.numpy as jnp
from jax import lax
from jax.experimental import pallas as pl
from jax.experimental.pallas import tpu as pltpu
from jax.sharding import PartitionSpec as P

MEMBERS = 256
NOBS = 512
BAT = 32
TOP = 3
PTS = 8
ITERS = 6
HALF = 128
MESH = pl.DeviceIdType.MESH
F32 = jnp.float32
BF16 = jnp.bfloat16
COPIES = 60
GROUP = 8
CENTRE = MEMBERS - 1


def iota(shape, dim):
    return lax.broadcasted_iota(jnp.int32, shape, dim)


def dot(a, b):
    return jnp.dot(a, b, preferred_element_type=F32)


def dot_last(a, b):
    return lax.dot_general(a, b, (((1,), (1,)), ((), ())), preferred_element_type=F32)


def flip(x, z, dim):
    if dim == 0:
        return x + 1 - 2 * (x % 2), z
    if dim == 1:
        return 3 - x, z
    if dim == 2:
        return x, z + 1 - 2 * (z % 2)
    return x, 3 - z


def gray_bits(x, z):
    high_x, high_z = x // 2, z // 2
    low_x, low_z = (x % 2 + high_x) % 2, (z % 2 + high_z) % 2
    return (low_x, high_x, low_z, high_z)


def root_iteration(phi_s, low_s, xi_s, scal, k):
    four, last = range(4), k == ITERS - 1
    f = [1.5 - 0.5 * scal[p][0] for p in four]
    m_new = [scal[p][0] * f[p] * f[p] for p in four]
    back = [-0.5 * scal[p][0] / f[p] for p in four]
    if not last:
        square = [dot(low_s[p], low_s[p]) for p in four]
    if k:
        grown = [dot(xi_s[p].astype(BF16), low_s[p]) for p in four]
    if not last:
        both = [((2.0 + back[p]) * phi_s[p] + square[p]).astype(BF16) for p in four]
        cubic = [dot(both[p], low_s[p]) for p in four]
    for p in four:
        xi_s[p] = (xi_s[p] + phi_s[p]) + grown[p] if k else phi_s[p]
    if not last:
        for p in four:
            ratio = f[p] * f[p] * f[p] / (1.5 - 0.5 * m_new[p])
            phi_new = (ratio * (1.0 + 2.0 * back[p])) * phi_s[p] + ratio * cubic[p]
            phi_s[p] = phi_new
            low_s[p] = phi_new.astype(BF16)
    return [(m_new[p], scal[p][1] * f[p]) for p in four]


def step_kernel(
    owner_h,
    points_h,
    count_h,
    len_h,
    weight_h,
    innov_h,
    taper_h,
    pert_h,
    back_h,
    stencil_h,
    frac_h,
    out_ref,
    pert,
    weight,
    innov,
    taper,
    owner_v,
    points_v,
    count_v,
    len_s,
    back,
    stencil,
    frac,
    wide_w,
    wide_i,
    source_v,
    source_s,
    coef,
    held,
    coef_n,
    coef_d,
    send3,
    recv3,
    send4,
    recv4,
    mine1,
    total,
    xheld,
    xsend3,
    xrecv3,
    xsend4,
    xrecv4,
    xmine1,
    xtotal,
    e_s,
    eb_s,
    z_s,
    window,
    rims,
    lhs_s,
    xlhs_s,
    cells,
    mean_s,
    mixed,
    done,
    small_sems,
    pert_sems,
    first_send,
    first_recv,
    send_sems,
    recv_sems,
):
    lat, lon = lax.axis_index("lat"), lax.axis_index("lon")
    x, z = lon // 4, lon % 4
    odd = lat % 2
    lead = (odd, 1 - odd)

    def to(dim):
        hx, hz = flip(x, z, dim % 4)
        return (lat, hx * 4 + hz)

    east, west = (lat, (lon + 1) % 16), (lat, (lon + 15) % 16)
    outer, inner = ((lat + 7 + 2 * odd) % 8, lon), (lat + 1 - 2 * odd, lon)

    barrier = pltpu.get_barrier_semaphore()
    peers = [to(d) for d in range(4)] + [east, west, outer, inner]
    for peer in peers:
        pl.semaphore_signal(barrier, inc=1, device_id=peer, device_id_type=MESH)

    small = []
    for n, (src, dst) in enumerate(
        (
            (owner_h, owner_v),
            (points_h, points_v),
            (count_h, count_v),
            (taper_h, taper),
            (len_h, len_s),
            (weight_h, weight),
            (innov_h, innov),
            (stencil_h, stencil),
            (frac_h, frac),
            (back_h, back),
        )
    ):
        small.append(pltpu.make_async_copy(src, dst, small_sems.at[n]))
    for c in small[:7]:
        c.start()
    fetches = []
    for g in range(BAT // GROUP):
        rows = pl.ds(g * GROUP, GROUP)
        fetches.append(pltpu.make_async_copy(pert_h.at[rows], pert.at[rows], pert_sems.at[g]))
        fetches[g].start()
    for c in small[7:]:
        c.start()

    for c in small[:4]:
        c.wait()
    owner_row = owner_v[...]
    turned = jnp.broadcast_to(owner_row, (BAT, BAT)).T
    before = (turned == owner_row) & (iota((BAT, BAT), 0) < iota((BAT, BAT), 1))
    rank_row = jnp.sum(jnp.where(before, 1, 0), axis=0, keepdims=True)
    mine = gray_bits(x, z)
    theirs = gray_bits(owner_row // 4, owner_row % 4)
    rel_row = jnp.zeros((1, BAT), jnp.int32)
    for d in range(4):
        rel_row = rel_row + ((theirs[d] + mine[d]) % 2) * (1 << d)
    slots = iota((HALF, BAT), 0)
    slot_rows = jnp.broadcast_to(rel_row * 4 + rank_row, (BAT, BAT)).T
    fills = jnp.broadcast_to(slot_rows[:, 0:1], (BAT, HALF)) == iota((BAT, HALF), 1)
    source = jnp.sum(jnp.where(fills, iota((BAT, HALF), 0), 0), axis=0, keepdims=True)
    source_v[...] = jnp.broadcast_to(source, (PTS, HALF))
    table = pltpu.make_async_copy(source_v, source_s, small_sems.at[10])
    table.start()
    points, listed = points_v[...], taper[...].astype(F32)
    q = iota((PTS, BAT), 0)
    point = jnp.where(
        q < 4, (q // 2) * 4 + (q % 2) * 3, ((q - 4) // 2) * 4 + 1 + q % 2
    )
    weights = jnp.zeros((PTS, BAT), F32)
    for j in range(TOP):
        hit = (point == points[j : j + 1, :]) & (count_v[...] > j)
        weights = weights + jnp.where(hit, listed[j : j + 1, :], 0.0)
    spot = jnp.where(slots == owner_row * 4 + rank_row, 1.0, 0.0).astype(BF16)
    coef[...] = dot_last(weights.astype(BF16), spot)
    for c in small[4:7]:
        c.wait()
    wide_w[...] = weight[...].astype(F32)
    wide_i[...] = innov[...].astype(F32)
    table.wait()
    pl.semaphore_wait(barrier, len(peers))

    used = []

    def push(src, dst, peer):
        n = len(used)
        c = pltpu.make_async_remote_copy(
            src_ref=src,
            dst_ref=dst,
            send_sem=send_sems.at[n],
            recv_sem=recv_sems.at[n],
            device_id=peer,
            device_id_type=MESH,
        )
        c.start()
        used.append(c)
        return c

    def first_copy(k, at):
        return pltpu.make_async_remote_copy(
            src_ref=held.at[k, at + 8, :, 0],
            dst_ref=held.at[k, at, :, 1],
            send_sem=first_send.at[k, at],
            recv_sem=first_recv.at[k, at],
            device_id=to(k),
            device_id_type=MESH,
        )

    row, col = iota((HALF, HALF), 0), iota((HALF, HALF), 1)
    tail_row = iota((16, NOBS), 0)
    for c in fetches:
        c.wait()

    def one_owner(n, carry):
        rel = 15 - n
        bits = [(rel // (1 << d)) % 2 for d in range(4)]
        place = [
            bits[k] * 8 + bits[(k + 1) % 4] * 4 + bits[(k + 2) % 4] * 2 + bits[(k + 3) % 4]
            for k in range(4)
        ]
        kinds = []
        for s in range(4):
            b = jnp.minimum(jnp.maximum(source_s[0, rel * 4 + s], 0), BAT - 1)
            p = pert[b]
            live = iota((1, NOBS), 1) < len_s[0, b]
            w = jnp.where(live, wide_w[pl.ds(b, 1), :], 0.0)
            wi = w * wide_i[pl.ds(b, 1), :]
            high = wi.astype(BF16).astype(F32)
            tail = jnp.where(tail_row == 0, high, jnp.where(tail_row == 1, wi - high, 0.0))
            scaled = p.T * w.astype(BF16)
            acc = dot(jnp.concatenate([scaled, tail.astype(BF16)], axis=0), p)
            corner = acc[HALF:256, HALF:256]
            left = jnp.where(col >= row, acc[0:HALF, 0:HALF], corner)
            top = jnp.concatenate([left, acc[0:HALF, HALF:256]], axis=1).astype(BF16)
            for k in range(4):
                for rc in range(2):
                    at = 32 * k + 16 * rc
                    held[k, place[k], rc, 0, s] = top[at : at + 16, :]
            proj = acc[256:257, :] + acc[257:258, :]
            diagonal = jnp.sum(jnp.where(col == row, corner, 0.0), axis=0, keepdims=True)
            kinds += [diagonal, proj[:, 0:HALF], proj[:, HALF:256], jnp.zeros((1, HALF), F32)]
        xheld[place[0], 0] = jnp.concatenate(kinds, axis=0).astype(BF16)
        for k in range(4):

            @pl.when(bits[k] == 1)
            def _():
                first_copy(k, place[k] % 8).start()

        return carry

    cn = [push(coef, coef_n.at[k], to(k)) for k in range(4)]
    lax.fori_loop(0, 16, one_owner, 0)
    x1 = push(xheld.at[8:16, 0], xheld.at[0:8, 1], to(0))
    for k in range(4):
        cn[k].wait_recv()
    cd = [push(coef_n.at[k], coef_d.at[k], to(k + 1)) for k in range(4)]

    def sources(k):
        rows = [coef[...], coef_n[k], coef_n[(k + 1) % 4], coef_d[k]]
        return jnp.concatenate(rows, axis=0).astype(BF16)

    def served(k, pos):
        sx, sz = x, z
        if pos & 2:
            sx, sz = flip(sx, sz, (k + 2) % 4)
        if pos & 1:
            sx, sz = flip(sx, sz, (k + 3) % 4)
        return sx * 4 + sz

    def spread(k, pos, width, each):
        lane = iota((HALF, width), 1)
        pick = jnp.where(
            iota((HALF, width), 0) == served(k, pos) * 4 + (lane // each) % 4, 1.0, 0.0
        ).astype(BF16)
        every = dot(sources(k), pick)
        lane8 = iota((8, width), 1) // (4 * each)
        out = jnp.zeros((8, width), F32)
        for j in range(4):
            out = out + jnp.where(lane8 == j, every[8 * j : 8 * j + 8, :], 0.0)
        return out

    def expand(weights, rows, each):
        width = weights.shape[1]
        keep = iota((rows, width), 1) % each == iota((rows, width), 0)
        blocks = [
            jnp.where(keep, jnp.broadcast_to(weights[p : p + 1, :], (rows, width)), 0.0)
            for p in range(PTS)
        ]
        return jnp.concatenate(blocks, axis=0).astype(BF16)

    def xmerged(pos):
        return dot(xlhs_s[pos][:, 0:64], xheld[pos].reshape(64, HALF))

    for k in range(4):
        cd[k].wait_recv()
    for pos in range(4):
        for k in range(4):
            lhs_s[k, pos] = expand(spread(k, pos, 256, 16), 16, 16)
        xlhs_s[pos] = expand(spread(0, pos, HALF, 4), 8, 4)

    s2a, s2b = [], []
    for k in range(4):
        for at in range(4, 8):
            first_copy(k, at).wait_recv()
        s2a.append(push(held.at[k, 6:8, :, 0:2], held.at[k, 2:4, :, 2:4], to(k + 1)))
    for k in range(4):
        s2b.append(push(held.at[k, 4:6, :, 0:2], held.at[k, 0:2, :, 2:4], to(k + 1)))
    x1.wait_recv()
    x2 = push(xheld.at[4:8, 0:2], xheld.at[0:4, 2:4], to(1))

    for c in small[7:]:
        c.wait()
    corner_id = (stencil[0] - (lat * 2 - 1)) * 6 + (stencil[1] - lon * 4 + 65) % 64
    fy, fx = frac[0], frac[1]
    corners = (
        (0, (1.0 - fy) * (1.0 - fx)),
        (6, fy * (1.0 - fx)),
        (1, (1.0 - fy) * fx),
        (7, fy * fx),
    )
    for t in range(4):
        turned = back[2 * t : 2 * t + 2].reshape(256, 256).T.astype(F32)
        mean = jnp.sum(turned, axis=0, keepdims=True) * (1.0 / MEMBERS)
        mean_s[t] = jnp.broadcast_to(mean, (8, 256))
        deviation = (turned - mean).astype(BF16).astype(F32)
        for j in range(24):
            value = jnp.zeros((8, HALF), F32)
            for add, share in corners:
                value = value + jnp.where(corner_id + add == j, share, 0.0)
            share = jnp.concatenate([value[2 * t : 2 * t + 1], value[2 * t + 1 : 2 * t + 2]], axis=1)
            cells[j, t] = (deviation * share).astype(BF16)

    for k in range(4):
        for at in range(4):
            first_copy(k, at).wait_recv()

    def merge(k, pos, g):
        lhs = lhs_s[k, pos, 64 * g : 64 * g + 64, :]
        return [dot(lhs, held[k, pos, rc].reshape(256, 256)).reshape(4, 16, 256) for rc in range(2)]

    def send_on(pos, g):
        for k in range(4):
            if (pos, g) == (3, 0):
                s2a[k].wait_recv()
            span = slice(4 * g, 4 * g + 4)
            for rc, value in enumerate(merge(k, pos, g)):
                send3[k, pos - 2, span, 16 * rc : 16 * rc + 16, :] = value.astype(BF16)
            s3[pos, g, k] = push(send3.at[k, pos - 2, span], recv3.at[k, pos - 2, span], to(k + 2))

    def keep_own(g):
        for k in range(4):
            if g == 0:
                s2b[k].wait_recv()
            span = slice(4 * g, 4 * g + 4)
            for rc, value in enumerate(merge(k, 1, g)):
                mine1[k, span, 16 * rc : 16 * rc + 16, :] = value
            for rc, value in enumerate(merge(k, 0, g)):
                at = 32 * k + 16 * rc
                total[span, at : at + 16, :] = value

    def last_step(g):
        for k in range(4):
            s3[3, g, k].wait_recv()
            span = slice(4 * g, 4 * g + 4)
            send4[k, span] = (mine1[k, span] + recv3[k, 1, span].astype(F32)).astype(BF16)
            s4[g, k] = push(send4.at[k, span], recv4.at[k, span], to(k + 3))

    s3, s4 = {}, {}
    send_on(3, 0)
    send_on(2, 0)
    x2.wait_recv()
    for pos in (3, 2):
        xsend3[pos - 2] = xmerged(pos).astype(BF16)
    x3 = push(xsend3, xrecv3, to(2))
    send_on(3, 1)
    keep_own(0)
    xmine1[...] = xmerged(1)
    xtotal[...] = xmerged(0)
    last_step(0)
    x3.wait_recv()
    xsend4[...] = (xmine1[...] + xrecv3[1].astype(F32)).astype(BF16)
    x4 = push(xsend4, xrecv4, to(3))
    send_on(2, 1)
    keep_own(1)
    for k in range(4):
        for at in range(8):
            first_copy(k, at).wait_send()
    early = 18
    for c in used[:early]:
        c.wait_send()
    last_step(1)
    late = len(used)
    x4.wait_recv()
    xtotal[...] += xrecv3[0].astype(F32) + xrecv4[...].astype(F32)

    outside, inside, side = [], [], []

    def rim(a, slot, column):
        if a == 0:
            outside.append((column, push(rims.at[slot], rims.at[18 * (1 - odd) + column], outer)))
        else:
            inside.append((column, push(rims.at[slot], rims.at[18 * odd + column], inner)))

    def unfold(n):
        fold = rims[n, 0:HALF, 0:HALF].astype(F32)
        right = rims[n, 0:HALF, HALF:256]
        turned = fold.T
        a = jnp.where(col >= row, fold, turned)
        c = jnp.where(col < row, fold, turned)
        last = rims[n, HALF:144, :]
        c = jnp.where(col == row, last[:, 0:HALF].astype(F32)[2:3, :], c)
        window[n, 0:HALF, :] = jnp.concatenate([a.astype(BF16), right], axis=1)
        window[n, HALF:256, :] = jnp.concatenate([right.T, c.astype(BF16)], axis=1)
        window[n, 256:272, :] = last

    def corners_on(a):
        for j in range(2):
            side[2 * a + j].wait_recv()
            column = 5 - 5 * j
            rim(a, (lead[a] + 1) * 6 + column, column)

    def gather(slots, start=False):
        for t in range(4):
            part = dot(window[slots[0]], cells[slots[0], t])
            for n in slots[1:]:
                part = part + dot(window[n], cells[n, t])
            mixed[t] = part if start else mixed[t] + part

    eye = jnp.where(row == col, float(CENTRE), 0.0)
    for g in range(2):
        scal, scales = [], []
        for k in range(4):
            s3[2, g, k].wait_recv()
            s4[g, k].wait_recv()
        for i in range(4):
            p = 4 * g + i
            for k in range(4):
                total[p, 32 * k : 32 * k + 32, :] += recv3[k, 0, p].astype(F32) + recv4[
                    k, p
                ].astype(F32)
            left, right = total[p, :, 0:HALF], total[p, :, HALF:256]
            turned = left.T
            a = jnp.where(col >= row, left, turned) + eye
            c = jnp.where(col < row, left, turned)
            c = jnp.where(col == row, xtotal[8 * p : 8 * p + 1, :], c) + eye
            square = jnp.sum(a * a + c * c + 2.0 * (right * right), keepdims=True)
            trace = jnp.sum(jnp.where(row == col, a + c, 0.0), keepdims=True)
            scale = jnp.sqrt(square)
            inverse = 1.0 / scale
            mean = trace * (1.0 / MEMBERS)
            off = jnp.where(row == col, mean, 0.0)
            slope = -0.5 * inverse / (1.5 - 0.5 * mean * inverse)
            a, c, b = (a - off) * slope, (c - off) * slope, right * slope
            e_s[i] = jnp.concatenate(
                [jnp.concatenate([a, b], axis=1), jnp.concatenate([b.T, c], axis=1)], axis=0
            )
            eb_s[i] = e_s[i].astype(BF16)
            scal.append((mean * inverse, jnp.ones((1, 1), F32)))
            scales.append(scale)
        for k in range(ITERS):
            scal = root_iteration(e_s, eb_s, z_s, scal, k)
        if g == 1:
            corners_on(0)
        big = iota((256, 256), 0) == iota((256, 256), 1)
        tail16 = iota((16, 256), 0)
        turns = []
        for a in range(2):
            for j in range(2):
                i = 2 * lead[a] + j
                flag = jnp.full((1, 1), lead[a], jnp.int32) == 1
                zd = jnp.where(flag, scal[2 + j][1], scal[j][1])
                scale = jnp.where(flag, scales[2 + j], scales[j])
                kinds = xtotal[pl.ds(pl.multiple_of(8 * (4 * g + i), 8), 8), :]
                shift = jnp.concatenate([kinds[1:2], kinds[2:3]], axis=1)
                turns.append([a, j, i, zd, scale, shift])
        for again in range(2):
            moved = []
            for a, j, i, zd, scale, v in turns:
                r = z_s[i]
                high = r.astype(BF16)
                low = (r - high.astype(F32)).astype(BF16)
                vh = v.astype(BF16).astype(F32)
                both = jnp.where(tail16 == 0, vh, jnp.where(tail16 == 1, v - vh, 0.0)).astype(BF16)
                moved.append(dot(both, high) + dot(both, low))
            for n, w in enumerate(moved):
                turns[n][5] = turns[n][3] * (turns[n][5] + w[0:1, :] + w[1:2, :])
        for a, j, i, zd, scale, v in turns:
            mw = v / scale
            amp = jnp.sqrt(float(CENTRE) / scale)
            whole = (amp * zd) * (z_s[i] + jnp.where(big, 1.0, 0.0))
            column = 1 + 3 * j if g == 0 else 2 + j
            slot = (lead[a] + 1) * 6 + column
            window[slot, 0:256, :] = whole.astype(BF16)
            corner = whole[HALF:256, HALF:256]
            fold = jnp.where(col >= row, whole[0:HALF, 0:HALF], corner)
            rims[slot, 0:HALF, :] = jnp.concatenate([fold, whole[0:HALF, HALF:256]], axis=1).astype(
                BF16
            )
            diagonal = jnp.sum(jnp.where(col == row, corner, 0.0), axis=0, keepdims=True)
            diagonal = jnp.concatenate([diagonal, jnp.zeros((1, HALF), F32)], axis=1)
            high = mw.astype(BF16).astype(F32)
            last = jnp.where(tail16 == 2, diagonal, 0.0)
            last = jnp.where(tail16 == 0, high, jnp.where(tail16 == 1, mw - high, last)).astype(BF16)
            rims[slot, HALF:144, :] = last
            window[slot, 256:272, :] = last
            if g == 0:
                across = rims.at[(lead[a] + 1) * 6 + 5 - 5 * j]
                side.append(push(rims.at[slot], across, west if j == 0 else east))
            rim(a, slot, column)

    corners_on(1)
    for n in (6, 11, 12, 17):
        unfold(n)
    gather([6 * r + c for r in (1, 2) for c in range(6)], start=True)
    for c in used[early:late]:
        c.wait_send()
    for column, c in inside:
        c.wait_recv()
    near, far = 18 * (1 - odd), 18 * odd
    for column in range(6):
        unfold(near + column)
    gather([near + column for column in range(6)])
    for column, c in outside:
        if column not in (2, 3):
            c.wait_recv()
    for column in (0, 1, 4, 5):
        unfold(far + column)
    gather([far + column for column in (0, 1, 4, 5)])
    for column, c in outside:
        if column in (2, 3):
            c.wait_recv()
    for column in (2, 3):
        unfold(far + column)
    outs = []
    for t in range(4):
        part = mixed[t] + (
            dot(window[far + 2], cells[far + 2, t]) + dot(window[far + 3], cells[far + 3, t])
        )
        shared = part[256:257, :] + part[257:258, :] + mean_s[t][0:1, :]
        whole = (part[0:256, :] + shared).astype(BF16)
        done[2 * t : 2 * t + 2] = whole.T.reshape(2, HALF, 256)
        span = pl.ds(2 * t, 2)
        outs.append(pltpu.make_async_copy(done.at[span], out_ref.at[span], small_sems.at[t]))
        outs[t].start()
    for c in used[late:]:
        c.wait_send()
    for c in outs:
        c.wait()


def step(args):
    hbm = pl.BlockSpec(memory_space=pl.ANY)
    i32 = jnp.int32
    vm = pltpu.VMEM
    return pl.pallas_call(
        step_kernel,
        out_shape=jax.ShapeDtypeStruct((8, HALF, 256), BF16),
        in_specs=[hbm] * len(args),
        out_specs=hbm,
        scratch_shapes=[
            vm((BAT, NOBS, MEMBERS), BF16),
            vm((BAT, NOBS), BF16),
            vm((BAT, NOBS), BF16),
            vm((TOP, BAT), BF16),
            vm((1, BAT), i32),
            vm((TOP, BAT), i32),
            vm((1, BAT), i32),
            pltpu.SMEM((1, BAT), i32),
            vm((8, HALF, 256), BF16),
            vm((2, 8, HALF), i32),
            vm((2, 8, HALF), F32),
            vm((BAT, NOBS), F32),
            vm((BAT, NOBS), F32),
            vm((PTS, HALF), i32),
            pltpu.SMEM((PTS, HALF), i32),
            vm((PTS, HALF), F32),
            vm((4, 16, 2, 4, 4, 16, 256), BF16),
            vm((4, PTS, HALF), F32),
            vm((4, PTS, HALF), F32),
            vm((4, 2, PTS, 32, 256), BF16),
            vm((4, 2, PTS, 32, 256), BF16),
            vm((4, PTS, 32, 256), BF16),
            vm((4, PTS, 32, 256), BF16),
            vm((4, PTS, 32, 256), F32),
            vm((PTS, HALF, 256), F32),
            vm((16, 4, 16, HALF), BF16),
            vm((2, 64, HALF), BF16),
            vm((2, 64, HALF), BF16),
            vm((64, HALF), BF16),
            vm((64, HALF), BF16),
            vm((64, HALF), F32),
            vm((64, HALF), F32),
            vm((4, 256, 256), F32),
            vm((4, 256, 256), BF16),
            vm((4, 256, 256), F32),
            vm((24, 272, 256), BF16),
            vm((24, 144, 256), BF16),
            vm((4, 4, HALF, 256), BF16),
            vm((4, 64, HALF), BF16),
            vm((24, 4, 256, 256), BF16),
            vm((4, 8, 256), F32),
            vm((4, 272, 256), F32),
            vm((8, HALF, 256), BF16),
            pltpu.SemaphoreType.DMA((11,)),
            pltpu.SemaphoreType.DMA((BAT // GROUP,)),
            pltpu.SemaphoreType.DMA((4, 8)),
            pltpu.SemaphoreType.DMA((4, 8)),
            pltpu.SemaphoreType.DMA((COPIES,)),
            pltpu.SemaphoreType.DMA((COPIES,)),
        ],
        compiler_params=pltpu.CompilerParams(
            collective_id=0, has_side_effects=True, vmem_limit_bytes=67043328
        ),
        name="step",
    )(*args)


def on_device(
    obs_pert,
    obs_weight,
    innovation,
    batch_len,
    batch_owner,
    batch_points,
    batch_count,
    batch_taper,
    background,
    stencil,
    frac,
):
    return step(
        (
            batch_owner.T,
            batch_points.T,
            batch_count.reshape(1, BAT),
            batch_len,
            obs_weight,
            innovation,
            batch_taper.T,
            obs_pert,
            background,
            stencil,
            frac,
        )
    )


def solution(mesh):
    return jax.shard_map(
        on_device,
        mesh=mesh,
        in_specs=(
            P(("lat", "lon"), None, None),
            P(("lat", "lon"), None),
            P(("lat", "lon"), None),
            P(("lat", "lon"), None),
            P(("lat", "lon"), None),
            P(("lat", "lon"), None),
            P(("lat", "lon")),
            P(("lat", "lon"), None),
            P("lat", "lon", None),
            P(None, "lat", "lon"),
            P(None, "lat", "lon"),
        ),
        out_specs=P("lat", "lon", None),
        check_vma=False,
    )
```
